32 devices in a mesh: row: 16 (over z, x, core), col: 2 (over y).
Axes of the slice: x: 2, y: 2, z: 4, core: 2. Of those that a mesh axis runs over, the one named last changes fastest.
Arguments:
- species: float32 [2, 128, 128, 64], P(None, None, 'row', 'col'), may hold values from -6 to 6
- symbol_x: float32 [128], replicated, may hold values from 0.3 to 3
- symbol_y: float32 [128], replicated, may hold values from 0.3 to 3
- symbol_z: float32 [64], replicated, may hold values from 0.3 to 3
Outputs:
- spectrum: float32 [2, 128, 128, 64], P(None, 'row', 'col')
The draws below stay inside these ranges and needn't reach their ends.
All inputs are finite; a program needn't handle non-finite values.
Results may differ from the reference program's by a relative error of at most 0.00007.
Values sent between devices are 32-bit elements; how exact they have to be, the bound alone decides.
A program may use at most 64 MiB of HBM per device.

```python
import jax
import jax.numpy as jnp
from jax import lax

GRID_X = 128
GRID_Y = 128
GRID_Z = 64
FIELDS = 2


def level_of(own_key, extent, split, least, high):
    def one(position, shards_of):
        heights = jax.random.uniform(jax.random.fold_in(jax.random.fold_in(own_key, 6), position), (shards_of,), jnp.float32, least / len(split), high / len(split))
        return jnp.repeat(jnp.exp(heights), extent[position] // shards_of).reshape((-1,) + (1,) * (len(extent) - position - 1))

    level = one(*split[0])
    for cut in split[1:]:
        level = level * one(*cut)
    return level


def centred(rng, shape, scale, most, cuts=(), held_as=jnp.bfloat16):
    entries = jax.random.normal(rng, shape, jnp.float32) * scale
    if len(cuts) > 0:
        entries = level_of(rng, shape, cuts, -0.22, 0.18) * entries
    return jnp.clip(entries, min=-most, max=most).astype(held_as)


def setup_inputs(seed: int = 0) -> dict:
    key_of = jax.random.split(jax.random.key(seed), 5)
    return {
        "species": centred(key_of[0], (FIELDS, GRID_X, GRID_Y, GRID_Z), 1.0, 6.0, ((2, 16), (3, 2)), jnp.float32),
        "symbol_x": jnp.clip(jax.random.uniform(key_of[1], (GRID_X,), jnp.float32, 0.3, 3.0), 0.3, 3.0),
        "symbol_y": jnp.clip(jax.random.uniform(key_of[2], (GRID_Y,), jnp.float32, 0.3, 3.0), 0.3, 3.0),
        "symbol_z": jnp.clip(jax.random.uniform(key_of[3], (GRID_Z,), jnp.float32, 0.3, 3.0), 0.3, 3.0),
    }


def basis_table(count):
    rank = jnp.arange(count)
    angle = (jnp.pi / (4 * count)) * (((2 * rank[:, None] + 1) * (2 * rank[None, :] + 1)) % (8 * count)).astype(jnp.float32)
    return jnp.cos(angle) * (2.0 / count) ** 0.5


def to_modes(values, dim):
    moved = jnp.tensordot(values, basis_table(values.shape[dim]), axes=([dim], [0]), precision=lax.Precision.HIGHEST)
    return jnp.moveaxis(moved, -1, dim)


def reference(species, symbol_x, symbol_y, symbol_z):
    spectrum = species
    spectrum = to_modes(spectrum, 1)
    spectrum = to_modes(spectrum, 2)
    spectrum = to_modes(spectrum, 3)
    symbol = symbol_x[:, None, None] + symbol_y[None, :, None] + symbol_z[None, None, :]
    spectrum = spectrum / symbol
    return spectrum
```

```python
import functools

import jax
import jax.numpy as jnp
import ml_dtypes
import numpy as np
from jax import lax
from jax.experimental import pallas as pl
from jax.experimental.pallas import tpu as pltpu
from jax.sharding import PartitionSpec as P

LANES = 128
CUTS = 2
GROUP = 4
F32, BF16 = jnp.float32, jnp.bfloat16
MESH = pl.DeviceIdType.MESH


def basis_table(count):
    odd = 2 * np.arange(count) + 1
    angle = np.pi / (4 * count) * (odd[:, None] * odd[None, :] % (8 * count))
    return np.cos(angle) * (2.0 / count) ** 0.5


def halves(table):
    high = table.astype(ml_dtypes.bfloat16)
    low = (table - high.astype(np.float64)).astype(ml_dtypes.bfloat16)
    return high, low


def split(values):
    high = values.astype(BF16)
    low = (values - high.astype(F32)).astype(BF16)
    return high, low


def tables(nx, ny, nz, share_z):
    width = LANES // share_z
    lane = np.arange(nx)
    group, rest = lane // LANES, lane % LANES
    order = width * (group * share_z + rest % share_z) + rest // share_z
    high, low = halves(basis_table(nx)[:, order])
    table_x = np.block([[high, low], [high, low]])
    high, low = halves(basis_table(ny))
    table_y = np.block([[high, high], [low, low]])
    eye = np.eye(width)
    wide = np.concatenate(
        [np.kron(eye, part) for part in np.split(basis_table(nz), nz // share_z, axis=0)], axis=0
    )
    table_z = np.stack(halves(wide))
    return table_x, table_y, table_z


def kernel(
    rows, cols, names,
    species, hx_hbm, hy_hbm, sx_hbm, sy_hbm, sz_hbm,
    lines, scale,
    xin, hx, hy, sx, sy, sz, send, recv, mixed, tall_x, tall_y,
    in_sem, row_send, row_recv, col_send, col_recv, row_ready, col_ready,
):
    row_name, col_name = names
    fields, share_y, share_z, nx = species.shape
    ny = rows * share_y
    nz = sz.shape[1]
    share_x, half_y = nx // rows, ny // cols
    width = LANES // share_z
    quads = share_x // width
    wide = quads * LANES // CUTS
    pieces = fields * CUTS
    groups = row_ready.shape[0]
    me, my_col = lax.axis_index(row_name), lax.axis_index(col_name)

    loads = [pltpu.make_async_copy(species.at[f], xin.at[f], in_sem.at[f]) for f in range(fields)]
    pairs = ((hx_hbm, hx), (hy_hbm, hy), (sx_hbm, sx), (sy_hbm, sy), (sz_hbm, sz))
    fetches = [
        pltpu.make_async_copy(a, b, in_sem.at[fields + i]) for i, (a, b) in enumerate(pairs)
    ]
    loads[0].start()
    fetches[0].start()
    for copy in loads[1:]:
        copy.start()

    barrier = pltpu.get_barrier_semaphore()

    def greet_row(t, carry):
        pl.semaphore_signal(barrier, inc=1, device_id={row_name: t}, device_id_type=MESH)
        return carry

    def greet_col(t, carry):
        pl.semaphore_signal(barrier, inc=1, device_id={col_name: t}, device_id_type=MESH)
        return carry

    lax.fori_loop(me + 1, rows, greet_row, 0)
    lax.fori_loop(my_col + 1, cols, greet_col, 0)
    for copy in fetches[1:]:
        copy.start()

    @pl.when(me + my_col > 0)
    def _():
        with jax.named_scope("barrier"):
            pl.semaphore_wait(barrier, me + my_col)

    def ready_row(t, carry):
        pl.semaphore_signal(
            row_ready.at[me // GROUP], inc=1, device_id={row_name: t}, device_id_type=MESH
        )
        return carry

    def ready_col(t, carry):
        pl.semaphore_signal(col_ready, inc=1, device_id={col_name: t}, device_id_type=MESH)
        return carry

    lax.fori_loop(0, me, ready_row, 0)
    lax.fori_loop(0, my_col, ready_col, 0)

    lane = lax.broadcasted_iota(jnp.int32, (share_y, LANES), 1)

    def row_copy(piece, target):
        return pltpu.make_async_remote_copy(
            src_ref=send.at[piece, target],
            dst_ref=recv.at[piece, me],
            send_sem=row_send.at[piece],
            recv_sem=row_recv.at[piece],
            device_id={row_name: target},
            device_id_type=MESH,
        )

    def row_all(piece):
        return pltpu.make_async_remote_copy(
            src_ref=send.at[piece, pl.ds(0, rows - 1)],
            dst_ref=recv.at[piece, pl.ds(0, rows - 1)],
            send_sem=row_send.at[piece],
            recv_sem=row_recv.at[piece],
            device_id={row_name: me},
            device_id_type=MESH,
        )

    def col_copy(piece, target):
        return pltpu.make_async_remote_copy(
            src_ref=mixed.at[piece, target],
            dst_ref=lines.at[piece, my_col],
            send_sem=col_send.at[piece],
            recv_sem=col_recv.at[piece],
            device_id={col_name: target},
            device_id_type=MESH,
        )

    def col_all(piece):
        return pltpu.make_async_remote_copy(
            src_ref=mixed.at[piece, pl.ds(0, cols - 1)],
            dst_ref=lines.at[piece, pl.ds(0, cols - 1)],
            send_sem=col_send.at[piece],
            recv_sem=col_recv.at[piece],
            device_id={col_name: my_col},
            device_id_type=MESH,
        )

    for f in range(fields):
        with jax.named_scope(f"load{f}"):
            loads[f].wait()
            if f == 0:
                fetches[0].wait()
        high, low = split(
            jnp.concatenate(
                [xin[f, :, z, :] for z in range(share_z)], axis=0
            )
        )
        both = jnp.dot(
            jnp.concatenate([high, low], axis=1), hx[...], preferred_element_type=F32
        )
        both = both[:, :nx] + both[:, nx:]
        for group in range(nx // LANES):
            tiles = [
                both[z * share_y : (z + 1) * share_y, group * LANES : (group + 1) * LANES]
                for z in range(share_z)
            ]
            bit = 1
            while bit < share_z:
                keep = (lane & bit) == 0
                for i in range(share_z):
                    if i & bit == 0:
                        a, b = tiles[i], tiles[i + bit]
                        tiles[i] = jnp.where(keep, a, pltpu.roll(b, bit, 1))
                        tiles[i + bit] = jnp.where(keep, pltpu.roll(a, LANES - bit, 1), b)
                bit *= 2
            for i in range(share_z):
                q = group * share_z + i
                target, at = q // quads, q % quads * LANES
                send[f * CUTS + at // wide, target, :, at % wide : at % wide + LANES] = tiles[i]
        with jax.named_scope(f"lower{f}"):
            for cut in range(CUTS):
                piece = f * CUTS + cut

                def send_lower(t, carry, piece=piece):
                    row_copy(piece, t).start()
                    return carry

                lax.fori_loop(0, me, send_lower, 0)
                recv[piece, me] = send[piece, me]

    for g in range(groups):
        least, most = g * GROUP, min(rows, (g + 1) * GROUP)
        first = jnp.maximum(least, me + 1)

        @pl.when(first < most)
        def _():
            with jax.named_scope(f"ready{g}"):
                pl.semaphore_wait(row_ready.at[g], most - first)
            for piece in range(pieces):

                def send_higher(t, carry, piece=piece):
                    row_copy(piece, t).start()
                    return carry

                lax.fori_loop(first, most, send_higher, 0)

    for copy in fetches[1:]:
        copy.wait()
    tall_x[...] = jnp.broadcast_to(sx[...], (LANES, nx)).T
    tall_y[...] = jnp.broadcast_to(sy[...], (LANES, ny)).T
    part_y = tall_y[pl.ds(my_col * half_y, half_y), :1]
    for x in range(share_x):
        part_x = tall_x[pl.ds(me * share_x + x, 1), :1]
        at = x % width * nz
        scale[x // width, :, at : at + nz] = 1.0 / (part_x + part_y + sz[...])

    @pl.when(my_col < cols - 1)
    def _():
        pl.semaphore_wait(col_ready, cols - 1 - my_col)


    for piece in range(pieces):
        with jax.named_scope(f"rowwait{piece}"):
            row_all(piece).wait_recv()
        high, low = split(recv[piece].reshape(ny, wide))
        both = jnp.dot(
            hy[...], jnp.concatenate([high, low], axis=0), preferred_element_type=F32
        )
        both = both[:ny] + both[ny:]
        mixed[piece] = both.reshape(cols, half_y, wide)
        for k in range(1, cols):
            col_copy(piece, (my_col + k) % cols).start()
        lines[piece, my_col] = mixed[piece, my_col]

    for piece in range(pieces):
        with jax.named_scope(f"sendwait{piece}"):
            row_all(piece).wait_send()
        with jax.named_scope(f"colwait{piece}"):
            col_all(piece).wait_send()
            col_all(piece).wait_recv()


def last_kernel(lines, scale, wz, out, held, out_sem):
    pieces, cols, half_y, wide = lines.shape
    nz = out.shape[3]
    width = scale.shape[2] // nz
    copies = []
    for piece in range(pieces):
        f, cut = piece // CUTS, piece % CUTS
        for i in range(wide // LANES):
            quad = cut * (wide // LANES) + i
            line = jnp.concatenate(
                [lines[piece, c, :, i * LANES : (i + 1) * LANES] for c in range(cols)], axis=1
            )
            high, low = split(line)
            both = jnp.dot(
                jnp.concatenate([high, low], axis=0), wz[0], preferred_element_type=F32
            )
            done = both[:half_y] + both[half_y:]
            done = done + jnp.dot(high, wz[1], preferred_element_type=F32)
            done = done * scale[quad]
            for j in range(width):
                held[f, quad * width + j] = done[:, j * nz : (j + 1) * nz]
            span = pl.ds(quad * width, width)
            copy = pltpu.make_async_copy(held.at[f, span], out.at[f, span], out_sem.at[f, quad])
            copy.start()
            copies.append(copy)
    with jax.named_scope("outwait"):
        for copy in copies:
            copy.wait()


def on_device(rows, cols, species, symbol_x, symbol_y, symbol_z):
    fields, nx, share_y, share_z = species.shape
    ny, nz = symbol_y.shape[0], symbol_z.shape[0]
    share_x, half_y = nx // rows, ny // cols
    width = LANES // share_z
    pieces, wide = fields * CUTS, share_x // width * LANES // CUTS
    hx, hy, wz = (jnp.asarray(t) for t in tables(nx, ny, nz, share_z))
    dma = pltpu.SemaphoreType.DMA
    regular = pltpu.SemaphoreType.REGULAR
    width_z = width * nz
    vmem = pl.BlockSpec(memory_space=pltpu.VMEM)
    lines, scale = pl.pallas_call(
        functools.partial(kernel, rows, cols, ("row", "col")),
        out_shape=(
            jax.ShapeDtypeStruct((pieces, cols, half_y, wide), F32),
            jax.ShapeDtypeStruct((share_x // width, half_y, width_z), F32),
        ),
        in_specs=[pl.BlockSpec(memory_space=pl.ANY)] * 6,
        out_specs=(vmem, vmem),
        scratch_shapes=[
            pltpu.VMEM((fields, share_y, share_z, nx), F32),
            pltpu.VMEM(hx.shape, BF16),
            pltpu.VMEM(hy.shape, BF16),
            pltpu.VMEM((1, nx), F32),
            pltpu.VMEM((1, ny), F32),
            pltpu.VMEM((1, nz), F32),
            pltpu.VMEM((pieces, rows, share_y, wide), F32),
            pltpu.VMEM((pieces, rows, share_y, wide), F32),
            pltpu.VMEM((pieces, cols, half_y, wide), F32),
            pltpu.VMEM((nx, LANES), F32),
            pltpu.VMEM((ny, LANES), F32),
            dma((fields + 5,)),
            dma((pieces,)),
            dma((pieces,)),
            dma((pieces,)),
            dma((pieces,)),
            regular((pl.cdiv(rows, GROUP),)),
            regular,
        ],
        compiler_params=pltpu.CompilerParams(collective_id=0, has_side_effects=True, vmem_limit_bytes=16 * 2**20),
    )(
        *(pltpu.with_memory_space_constraint(v, pltpu.HBM) for v in (jnp.transpose(species, (0, 2, 3, 1)), hx, hy,
        symbol_x[None, :], symbol_y[None, :], symbol_z[None, :])),
    )
    shape = (fields, share_x, half_y, nz)
    return pl.pallas_call(
        last_kernel,
        out_shape=jax.ShapeDtypeStruct(shape, F32),
        in_specs=[vmem, vmem, vmem],
        out_specs=pl.BlockSpec(memory_space=pl.ANY),
        scratch_shapes=[pltpu.VMEM(shape, F32), dma((fields, share_x // width))],
        compiler_params=pltpu.CompilerParams(vmem_limit_bytes=16 * 2**20),
    )(lines, scale, wz)


def solution(mesh):
    rows, cols = mesh.shape["row"], mesh.shape["col"]
    in_specs = (P(None, None, "row", "col"), P(), P(), P())
    out_specs = P(None, "row", "col", None)
    return jax.shard_map(
        functools.partial(on_device, rows, cols),
        mesh=mesh, in_specs=in_specs, out_specs=out_specs, check_vma=False,
    )
```

```python
import functools

import jax
import jax.numpy as jnp
import ml_dtypes
import numpy as np
from jax import lax
from jax.experimental import pallas as pl
from jax.experimental.pallas import tpu as pltpu
from jax.sharding import PartitionSpec as P

LANES = 128
GROUP = 4
F32, BF16 = jnp.float32, jnp.bfloat16
MESH = pl.DeviceIdType.MESH


def basis_table(count):
    odd = 2 * np.arange(count) + 1
    angle = np.pi / (4 * count) * (odd[:, None] * odd[None, :] % (8 * count))
    return np.cos(angle) * (2.0 / count) ** 0.5


def halves(table):
    high = table.astype(ml_dtypes.bfloat16)
    low = (table - high.astype(np.float64)).astype(ml_dtypes.bfloat16)
    return high, low


def split(values):
    high = values.astype(BF16)
    low = (values - high.astype(F32)).astype(BF16)
    return high, low


def padded(count):
    return -(-count // LANES) * LANES


def tables(rows, nx, ny, nz, share_z):
    width, half = LANES // share_z, share_z // 2
    share_x = nx // rows
    lane = np.arange(LANES)
    blocks = []
    for quad in range(share_x // width):
        for first in range(0, rows, half):
            column = lane[: LANES // 2]
            x = (first + column % half) * share_x + quad * width + column // half
            high, low = halves(basis_table(nx)[:, x])
            blocks += [high, low]
    table_x = np.tile(np.concatenate(blocks, axis=1), (2, 1))
    high, low = halves(basis_table(ny))
    table_y = np.block([[high, high], [low, low]])
    wide = np.zeros((nz // share_z, LANES, width, padded(nz)))
    for start in range(nz // share_z):
        z = start * share_z + lane % half + half * (lane // (LANES // 2))
        wide[start, lane, lane % (LANES // 2) // half, :nz] = basis_table(nz)[z]
    table_z = np.stack(halves(wide.reshape(-1, width * padded(nz))))
    return table_x, table_y, table_z


def kernel(
    rows, cols, names,
    species, hx_hbm, hy_hbm, wz_hbm, sx_hbm, sy_hbm, sz_hbm,
    lines, scale, early,
    xin, mid, hx, hy, wz, sx, sy, sz, send, recv, mixed, gathered, tall_x, tall_y,
    in_sem, row_send, row_recv, col_send, col_recv, row_ready, col_ready,
):
    row_name, col_name = names
    fields, _, _, nx = species.shape
    ny, nz = sy.shape[1], sz.shape[1]
    share_y, share_z = ny // rows, nz // cols
    share_x, half_y = nx // rows, ny // cols
    width, half = LANES // share_z, share_z // 2
    quads = share_x // width
    pieces = fields * quads
    groups = row_ready.shape[0]
    middle = groups // 2 - 1
    me, my_col = lax.axis_index(row_name), lax.axis_index(col_name)
    mine = me // GROUP

    def fetch(source, target, semaphore, parts):
        step = source.shape[0] // parts
        for i in range(parts):
            span = pl.ds(i * step, step)
            pltpu.make_async_copy(source.at[span], target.at[span], semaphore).start()

    blocks = nx // LANES
    fetch(hx_hbm, hx, in_sem.at[0], 4)
    for f in range(fields):
        for b in range(blocks):
            for y in range(share_y):
                pltpu.make_async_copy(
                    species.at[f, y, :, pl.ds(b * LANES, LANES)], xin.at[f, b, :, y, :], in_sem.at[1 + f]
                ).start()

    barrier = pltpu.get_barrier_semaphore()

    def greet_row(t, carry):
        pl.semaphore_signal(barrier, inc=1, device_id={row_name: t}, device_id_type=MESH)
        return carry

    def greet_col(t, carry):
        pl.semaphore_signal(barrier, inc=1, device_id={col_name: t}, device_id_type=MESH)
        return carry

    is_middle = mine == middle
    past = mine == middle + 1
    back = (mine - 1) * GROUP
    lax.fori_loop(jnp.where(past, back, 0), jnp.where(past, back + GROUP, 0), greet_row, 0)
    lax.fori_loop(me + 1, rows, greet_row, 0)
    lax.fori_loop(my_col + 1, cols, greet_col, 0)
    rest = ((hy_hbm, hy), (wz_hbm, wz), (sx_hbm, sx), (sy_hbm, sy), (sz_hbm, sz))
    fetches = [
        pltpu.make_async_copy(a, b, in_sem.at[1 + fields + i]) for i, (a, b) in enumerate(rest)
    ]
    for copy in fetches:
        copy.start()

    def ready_row(t, carry):
        pl.semaphore_signal(row_ready.at[mine], inc=1, device_id={row_name: t}, device_id_type=MESH)
        return carry

    def ready_col(t, carry):
        pl.semaphore_signal(col_ready, inc=1, device_id={col_name: t}, device_id_type=MESH)
        return carry

    def meet():
        count = me + my_col + jnp.where(is_middle, GROUP, 0)

        @pl.when(count > 0)
        def _():
            with jax.named_scope("barrier"):
                pl.semaphore_wait(barrier, count)

        lax.fori_loop(0, jnp.where(past, back, me), ready_row, 0)
        lax.fori_loop(jnp.where(past, mine * GROUP, me), me, ready_row, 0)
        lax.fori_loop(0, my_col, ready_col, 0)

    soon = (me % GROUP >= GROUP // 2) & ~is_middle
    pl.when(soon)(meet)

    lane = lax.broadcasted_iota(jnp.int32, (share_y, LANES), 1)

    def row_copy(piece, target):
        return pltpu.make_async_remote_copy(
            src_ref=send.at[piece, target],
            dst_ref=recv.at[piece, me],
            send_sem=row_send.at[piece],
            recv_sem=row_recv.at[piece],
            device_id={row_name: target},
            device_id_type=MESH,
        )

    def row_all(piece):
        return pltpu.make_async_remote_copy(
            src_ref=send.at[piece, pl.ds(0, rows - 1)],
            dst_ref=recv.at[piece, pl.ds(0, rows - 1)],
            send_sem=row_send.at[piece],
            recv_sem=row_recv.at[piece],
            device_id={row_name: me},
            device_id_type=MESH,
        )

    def col_copy(piece, target):
        return pltpu.make_async_remote_copy(
            src_ref=mixed.at[piece, target],
            dst_ref=(gathered.at[piece, my_col] if piece < pieces - 1 else lines.at[my_col]),
            send_sem=col_send.at[piece],
            recv_sem=col_recv.at[piece],
            device_id={col_name: target},
            device_id_type=MESH,
        )

    def col_all(piece):
        part = pl.ds(0, cols - 1)
        return pltpu.make_async_remote_copy(
            src_ref=mixed.at[piece, part],
            dst_ref=(gathered.at[piece, part] if piece < pieces - 1 else lines.at[part]),
            send_sem=col_send.at[piece],
            recv_sem=col_recv.at[piece],
            device_id={col_name: my_col},
            device_id_type=MESH,
        )

    def send_to(least, most, some):
        for piece in some:

            def step(t, carry, piece=piece):
                row_copy(piece, t).start()
                return carry

            lax.fori_loop(least, most, step, 0)

    everything = range(pieces)
    front = jnp.minimum(mine, 1) * GROUP
    near_high = (mine + 2) * GROUP
    with jax.named_scope("load"):
        pltpu.make_async_copy(hx_hbm, hx, in_sem.at[0]).wait()
        for f in range(fields):
            pltpu.make_async_copy(xin.at[f], xin.at[f], in_sem.at[1 + f]).wait()
    for f in range(fields):
        cut = [
            split(xin[f, b].reshape(share_z * share_y, LANES)) for b in range(blocks)
        ]
        mid[f] = jnp.dot(
            jnp.concatenate([part for pair in zip(*cut) for part in pair], axis=1),
            hx[...],
            preferred_element_type=F32,
        )
    for piece in everything:
        f, quad = piece // quads, piece % quads
        for block in range(rows // half):
            at = (quad * (rows // half) + block) * LANES
            tiles = [
                mid[f, z * share_y : (z + 1) * share_y, at : at + LANES] for z in range(share_z)
            ]
            keep = lane < LANES // 2
            tiles = [
                jnp.where(keep, a, b) + pltpu.roll(jnp.where(keep, b, a), LANES // 2, 1)
                for a, b in zip(tiles[:half], tiles[half:])
            ]
            unit = 1
            while unit < half:
                radix = min(4, half // unit)
                place = lane // unit % radix
                turned = list(tiles)
                for i in range(half):
                    own = i // unit % radix
                    for other in range(radix):
                        source = tiles[i + (other - own) * unit]
                        if other != own:
                            source = pltpu.roll(source, (other - own) * unit % LANES, 1)
                        turned[i] = source if other == 0 else jnp.where(place == other, source, turned[i])
                tiles = turned
                unit *= radix
            for i in range(half):
                send[piece, block * half + i] = tiles[i]
        if quad < quads - 1:
            continue
        if f == 0:
            pl.when(~soon & ~is_middle)(meet)
        with jax.named_scope(f"near{f}"):

            @pl.when(~is_middle)
            def _():
                for some in range(f * quads, (f + 1) * quads):
                    send_to(0, front, [some])

            for some in range(f * quads, (f + 1) * quads):
                recv[some, me] = send[some, me]

    @pl.when(is_middle)
    def _():
        meet()
        for piece in everything:
            send_to(near_high - GROUP, near_high, [piece])
            send_to(0, front, [piece])

    send_to(front, me, everything)
    for g in [*range(middle), *range(middle + 1, groups), middle]:
        least, most = g * GROUP, (g + 1) * GROUP
        first = jnp.maximum(least, me + 1)

        @pl.when((first < most) & ~(is_middle & (mine == g - 1)))
        def _():
            with jax.named_scope(f"ready{g}"):
                pl.semaphore_wait(row_ready.at[g], most - first)
            send_to(first, most, everything)

    for copy in fetches:
        copy.wait()
    tall_x[...] = jnp.broadcast_to(sx[...], (LANES, nx)).T
    tall_y[...] = jnp.broadcast_to(sy[...], (LANES, ny)).T
    part_y = tall_y[pl.ds(my_col * half_y, half_y), :1]
    for x in range(share_x):
        part_x = tall_x[pl.ds(me * share_x + x, 1), :1]
        at = x % width * padded(nz)
        scale[x // width, :, at : at + nz] = 1.0 / (part_x + part_y + sz[...])

    @pl.when(my_col < cols - 1)
    def _():
        pl.semaphore_wait(col_ready, cols - 1 - my_col)

    for piece in everything:
        with jax.named_scope(f"rowwait{piece}"):
            row_all(piece).wait_recv()
        high, low = split(recv[piece].reshape(ny, LANES))
        both = jnp.dot(
            hy[...], jnp.concatenate([high, low], axis=0), preferred_element_type=F32
        )
        both = both[:ny] + both[ny:]
        mixed[piece] = both.reshape(cols, half_y, LANES)
        for k in range(1, cols):
            col_copy(piece, (my_col + k) % cols).start()
        if piece < pieces - 1:
            gathered[piece, my_col] = mixed[piece, my_col]
        else:
            lines[my_col] = mixed[piece, my_col]

    for piece in everything:
        with jax.named_scope(f"colwait{piece}"):
            row_all(piece).wait_send()
            col_all(piece).wait_send()
            col_all(piece).wait_recv()
        if piece < pieces - 1:
            last_axis(gathered.at[piece], scale[piece % quads], wz, early.at[piece])


def last_axis(lines, scale, wz, out):
    cols, half_y, _ = lines.shape
    width, _, nz = out.shape
    line = jnp.concatenate([lines[c] for c in range(cols)], axis=1)
    high, low = split(line)
    both = jnp.dot(jnp.concatenate([high, low], axis=0), wz[0], preferred_element_type=F32)
    done = both[:half_y] + both[half_y:]
    done = done + jnp.dot(high, wz[1], preferred_element_type=F32)
    done = done * scale
    for j in range(width):
        out[j] = done[:, j * padded(nz) : j * padded(nz) + nz]


def last_kernel(lines, scale, early, wz, out, held, out_sem):
    pieces = early.shape[0] + 1
    quads, width = scale.shape[0], held.shape[0]
    copies = []
    for piece in range(pieces):
        if piece == pieces - 1:
            last_axis(lines, scale[piece % quads], wz, held)
        source = early.at[piece] if piece < pieces - 1 else held
        place = out.at[piece // quads, pl.ds(piece % quads * width, width)]
        copy = pltpu.make_async_copy(source, place, out_sem.at[piece])
        copy.start()
        copies.append(copy)
    with jax.named_scope("outwait"):
        for copy in copies:
            copy.wait()


def on_device(rows, cols, species, symbol_x, symbol_y, symbol_z):
    fields, nx, share_y, share_z = species.shape
    ny, nz = symbol_y.shape[0], symbol_z.shape[0]
    share_x, half_y = nx // rows, ny // cols
    width = LANES // share_z
    quads = share_x // width
    pieces = fields * quads
    hx, hy, wz = (jnp.asarray(t) for t in tables(rows, nx, ny, nz, share_z))
    dma = pltpu.SemaphoreType.DMA
    regular = pltpu.SemaphoreType.REGULAR
    width_z = width * padded(nz)
    vmem = pl.BlockSpec(memory_space=pltpu.VMEM)
    lines, scale, early = pl.pallas_call(
        functools.partial(kernel, rows, cols, ("row", "col")),
        out_shape=(
            jax.ShapeDtypeStruct((cols, half_y, LANES), F32),
            jax.ShapeDtypeStruct((quads, half_y, width_z), F32),
            jax.ShapeDtypeStruct((pieces - 1, width, half_y, nz), F32),
        ),
        in_specs=[pl.BlockSpec(memory_space=pl.ANY)] * 7,
        out_specs=(vmem, vmem, vmem),
        scratch_shapes=[
            pltpu.VMEM((fields, nx // LANES, share_z, share_y, LANES), F32),
            pltpu.VMEM((fields, share_y * share_z, 2 * nx), F32),
            pltpu.VMEM(hx.shape, BF16),
            pltpu.VMEM(hy.shape, BF16),
            pltpu.VMEM(wz.shape, BF16),
            pltpu.VMEM((1, nx), F32),
            pltpu.VMEM((1, ny), F32),
            pltpu.VMEM((1, nz), F32),
            pltpu.VMEM((pieces, rows, share_y, LANES), F32),
            pltpu.VMEM((pieces, rows, share_y, LANES), F32),
            pltpu.VMEM((pieces, cols, half_y, LANES), F32),
            pltpu.VMEM((pieces - 1, cols, half_y, LANES), F32),
            pltpu.VMEM((nx, LANES), F32),
            pltpu.VMEM((ny, LANES), F32),
            dma((fields + 6,)),
            dma((pieces,)),
            dma((pieces,)),
            dma((pieces,)),
            dma((pieces,)),
            regular((rows // GROUP,)),
            regular,
        ],
        compiler_params=pltpu.CompilerParams(collective_id=0, has_side_effects=True, vmem_limit_bytes=24 * 2**20),
    )(
        *(pltpu.with_memory_space_constraint(v, pltpu.HBM) for v in (jnp.transpose(species, (0, 2, 3, 1)), hx, hy,
        wz, symbol_x[None, :], symbol_y[None, :], symbol_z[None, :])),
    )
    return pl.pallas_call(
        last_kernel,
        out_shape=jax.ShapeDtypeStruct((fields, share_x, half_y, nz), F32),
        in_specs=[vmem, vmem, vmem, vmem],
        out_specs=pl.BlockSpec(memory_space=pl.ANY),
        scratch_shapes=[pltpu.VMEM((width, half_y, nz), F32), dma((pieces,))],
        compiler_params=pltpu.CompilerParams(vmem_limit_bytes=24 * 2**20),
    )(lines, scale, early, wz)


def solution(mesh):
    rows, cols = mesh.shape["row"], mesh.shape["col"]
    in_specs = (P(None, None, "row", "col"), P(), P(), P())
    out_specs = P(None, "row", "col", None)
    return jax.shard_map(
        functools.partial(on_device, rows, cols),
        mesh=mesh, in_specs=in_specs, out_specs=out_specs, check_vma=False,
    )
```

```python
import functools

import jax
import jax.numpy as jnp
import ml_dtypes
import numpy as np
from jax import lax
from jax.experimental import pallas as pl
from jax.experimental.pallas import tpu as pltpu
from jax.sharding import PartitionSpec as P

LANES = 128
GROUP = 4
F32, BF16 = jnp.float32, jnp.bfloat16
MESH = pl.DeviceIdType.MESH


def basis_table(count):
    odd = 2 * np.arange(count) + 1
    angle = np.pi / (4 * count) * (odd[:, None] * odd[None, :] % (8 * count))
    return np.cos(angle) * (2.0 / count) ** 0.5


def halves(table):
    high = table.astype(ml_dtypes.bfloat16)
    low = (table - high.astype(np.float64)).astype(ml_dtypes.bfloat16)
    return high, low


def split(values):
    high = values.astype(BF16)
    low = (values - high.astype(F32)).astype(BF16)
    return high, low


def padded(count):
    return -(-count // LANES) * LANES


def tables(rows, nx, ny, nz, share_z):
    width, half = LANES // share_z, share_z // 2
    share_x = nx // rows
    lane = np.arange(LANES)
    blocks = []
    for quad in range(share_x // width):
        for first in range(0, rows, half):
            column = lane[: LANES // 2]
            x = (first + column % half) * share_x + quad * width + column // half
            high, low = halves(basis_table(nx)[:, x])
            blocks += [high, low]
    table_x = np.tile(np.concatenate(blocks, axis=1), (2, 1))
    high, low = halves(basis_table(ny))
    table_y = np.block([[high, high], [low, low]])
    wide = np.zeros((nz // share_z, LANES, width, padded(nz)))
    for start in range(nz // share_z):
        z = start * share_z + lane % half + half * (lane // (LANES // 2))
        wide[start, lane, lane % (LANES // 2) // half, :nz] = basis_table(nz)[z]
    table_z = np.stack(halves(wide.reshape(-1, width * padded(nz))))
    return table_x, table_y, table_z


def kernel(
    rows, cols, names,
    species, hx_hbm, hy_hbm, wz_hbm, sx_hbm, sy_hbm, sz_hbm,
    lines, scale, early,
    xin, mid, hx, hy, wz, sx, sy, sz, send, recv, mixed, gathered, tall_x, tall_y,
    in_sem, row_send, row_recv, col_send, col_recv, row_ready,
):
    row_name, col_name = names
    fields, _, _, nx = species.shape
    ny, nz = sy.shape[1], sz.shape[1]
    share_y, share_z = ny // rows, nz // cols
    share_x, half_y = nx // rows, ny // cols
    width, half = LANES // share_z, share_z // 2
    quads = share_x // width
    pieces = fields * quads
    groups = rows // GROUP
    middle = groups // 2 - 1
    me, my_col = lax.axis_index(row_name), lax.axis_index(col_name)
    mine = me // GROUP

    def fetch(source, target, semaphore, parts):
        step = source.shape[0] // parts
        for i in range(parts):
            span = pl.ds(i * step, step)
            pltpu.make_async_copy(source.at[span], target.at[span], semaphore).start()

    blocks = nx // LANES
    fetch(hx_hbm, hx, in_sem.at[0], 4)
    for f in range(fields):
        for b in range(blocks):
            for y in range(share_y):
                pltpu.make_async_copy(
                    species.at[f, y, :, pl.ds(b * LANES, LANES)], xin.at[f, b, :, y, :], in_sem.at[f]
                ).start()

    barrier = pltpu.get_barrier_semaphore()

    def greet_row(t, carry):
        pl.semaphore_signal(barrier, inc=1, device_id={row_name: t}, device_id_type=MESH)
        return carry

    def greet_col(t, carry):
        pl.semaphore_signal(barrier, inc=1, device_id={col_name: t}, device_id_type=MESH)
        return carry

    low = mine <= middle
    back = (mine - 1) * GROUP
    past = (mine > 0) & (mine <= middle + 1)
    lax.fori_loop(jnp.where(past, back, 0), jnp.where(past, back + GROUP, 0), greet_row, 0)
    lax.fori_loop(me + 1, rows, greet_row, 0)
    lax.fori_loop(my_col + 1, cols, greet_col, 0)
    rest = ((hy_hbm, hy), (wz_hbm, wz), (sx_hbm, sx), (sy_hbm, sy), (sz_hbm, sz))
    fetches = [
        pltpu.make_async_copy(a, b, in_sem.at[fields]) for a, b in rest
    ]
    for copy in fetches:
        copy.start()

    def ready_row(t, carry):
        other = (~low & (t < (middle + 1) * GROUP)).astype(jnp.int32)
        pl.semaphore_signal(row_ready.at[other], inc=1, device_id={row_name: t}, device_id_type=MESH)
        return carry

    def ready_col(t, carry):
        pl.semaphore_signal(row_ready.at[0], inc=1, device_id={col_name: t}, device_id_type=MESH)
        return carry

    def meet():
        count = me + my_col + jnp.where(low, GROUP, 0)

        @pl.when(count > 0)
        def _():
            with jax.named_scope("barrier"):
                pl.semaphore_wait(barrier, count)

        lax.fori_loop(0, jnp.where(past, back, me), ready_row, 0)
        lax.fori_loop(jnp.where(past, mine * GROUP, me), me, ready_row, 0)
        lax.fori_loop(0, my_col, ready_col, 0)

    soon = (me % GROUP >= GROUP // 2) & ~low
    pl.when(soon)(meet)

    lane = lax.broadcasted_iota(jnp.int32, (share_y, LANES), 1)

    def row_copy(piece, target):
        return pltpu.make_async_remote_copy(
            src_ref=send.at[piece, target],
            dst_ref=recv.at[piece, me],
            send_sem=row_send,
            recv_sem=row_recv.at[piece],
            device_id={row_name: target},
            device_id_type=MESH,
        )

    def row_all(piece):
        return pltpu.make_async_remote_copy(
            src_ref=send.at[piece, pl.ds(0, rows - 1)],
            dst_ref=recv.at[piece, pl.ds(0, rows - 1)],
            send_sem=row_send,
            recv_sem=row_recv.at[piece],
            device_id={row_name: me},
            device_id_type=MESH,
        )

    def col_copy(piece, target):
        return pltpu.make_async_remote_copy(
            src_ref=mixed.at[piece, target],
            dst_ref=(gathered.at[piece, my_col] if piece < pieces - 1 else lines.at[my_col]),
            send_sem=col_send,
            recv_sem=col_recv.at[piece],
            device_id={col_name: target},
            device_id_type=MESH,
        )

    def col_all(piece):
        part = pl.ds(0, cols - 1)
        return pltpu.make_async_remote_copy(
            src_ref=mixed.at[piece, part],
            dst_ref=(gathered.at[piece, part] if piece < pieces - 1 else lines.at[part]),
            send_sem=col_send,
            recv_sem=col_recv.at[piece],
            device_id={col_name: my_col},
            device_id_type=MESH,
        )

    def send_to(least, most, some):
        for piece in some:

            def step(t, carry, piece=piece):
                row_copy(piece, t).start()
                return carry

            lax.fori_loop(least, most, step, 0)

    everything = range(pieces)
    front = jnp.minimum(mine, 1) * GROUP
    near_high = (mine + 2) * GROUP
    def product(f):
        cut = [
            split(xin[f, b].reshape(share_z * share_y, LANES)) for b in range(blocks)
        ]
        line = jnp.concatenate([part for pair in zip(*cut) for part in pair], axis=1)
        size = half * share_y
        for at in (0, size):
            mid[f, at : at + size] = jnp.dot(
                line[at : at + size], hx[...], preferred_element_type=F32
            )

    with jax.named_scope("load"):
        pltpu.make_async_copy(hx_hbm, hx, in_sem.at[0]).wait()
        for f in range(fields):
            pltpu.make_async_copy(xin.at[f], xin.at[f], in_sem.at[f]).wait()
    for f in range(fields):
        product(f)
    for piece in everything:
        f, quad = piece // quads, piece % quads
        for block in range(rows // half):
            at = (quad * (rows // half) + block) * LANES
            tiles = [
                mid[f, z * share_y : (z + 1) * share_y, at : at + LANES] for z in range(share_z)
            ]
            keep = lane < LANES // 2
            tiles = [
                jnp.where(keep, a, b) + pltpu.roll(jnp.where(keep, b, a), LANES // 2, 1)
                for a, b in zip(tiles[:half], tiles[half:])
            ]
            unit = 1
            while unit < half:
                radix = min(4, half // unit)
                place = lane // unit % radix
                turned = list(tiles)
                for i in range(half):
                    own = i // unit % radix
                    for other in range(radix):
                        source = tiles[i + (other - own) * unit]
                        if other != own:
                            source = pltpu.roll(source, (other - own) * unit % LANES, 1)
                        turned[i] = source if other == 0 else jnp.where(place == other, source, turned[i])
                tiles = turned
                unit *= radix
            for i in range(half):
                send[piece, block * half + i] = tiles[i]
        if quad < quads - 1:
            continue
        if f == 0:
            pl.when(~soon & ~low)(meet)
        with jax.named_scope(f"near{f}"):

            @pl.when(~low)
            def _():
                for some in range(f * quads, (f + 1) * quads):
                    send_to(0, front, [some])

            for some in range(f * quads, (f + 1) * quads):
                recv[some, me] = send[some, me]

    @pl.when(low)
    def _():
        meet()
        for piece in everything:
            send_to(0, front, [piece])
            send_to(near_high - GROUP, near_high, [piece])

    across = (jnp.where(mine > 0, GROUP, 0), jnp.minimum(mine, middle + 1) * GROUP)
    pl.when(mine <= middle + 1)(lambda: send_to(*across, everything))
    for g in reversed(range(middle + 1, groups)):

        @pl.when(g < mine)
        def _():
            send_to(g * GROUP, (g + 1) * GROUP, everything)

    pl.when(mine > middle + 1)(lambda: send_to(*across, everything))
    send_to(mine * GROUP, me, everything)

    half_end = jnp.where(low, (middle + 1) * GROUP, rows)
    last = jnp.minimum((mine + 1) * GROUP, half_end)
    greeted = jnp.where(low, jnp.minimum((mine + 2) * GROUP, half_end), last)
    count = half_end - me - 1 - (greeted - last) + cols - 1 - my_col

    @pl.when(count > 0)
    def _():
        with jax.named_scope("ready0"):
            pl.semaphore_wait(row_ready.at[0], count)

    send_to(me + 1, last, everything)
    send_to(greeted, half_end, everything)

    @pl.when(low)
    def _():
        far = jnp.maximum(mine + 2, middle + 1) * GROUP
        with jax.named_scope("ready1"):
            pl.semaphore_wait(row_ready.at[1], rows - far)
        send_to(far, rows, everything)

    for copy in fetches:
        copy.wait()
    tall_x[...] = jnp.broadcast_to(sx[...], (LANES, nx)).T
    tall_y[...] = jnp.broadcast_to(sy[...], (LANES, ny)).T
    part_y = tall_y[pl.ds(my_col * half_y, half_y), :1]
    for x in range(share_x):
        part_x = tall_x[pl.ds(me * share_x + x, 1), :1]
        at = x % width * padded(nz)
        scale[x // width, :, at : at + nz] = 1.0 / (part_x + part_y + sz[...])

    for piece in everything:
        with jax.named_scope(f"rowwait{piece}"):
            row_all(piece).wait_recv()
        high, low = split(recv[piece].reshape(ny, LANES))
        stacked = jnp.concatenate([high, low], axis=0)
        parts = []
        for k in range(1, cols + 1):
            at = pl.multiple_of((my_col + k) % cols * half_y, half_y)
            table = jnp.concatenate([hy[pl.ds(at, half_y), :], hy[pl.ds(ny + at, half_y), :]], axis=0)
            both = jnp.dot(table, stacked, preferred_element_type=F32)
            parts.append(both[:half_y] + both[half_y:])
        for k in range(1, cols):
            mixed[piece, (my_col + k) % cols] = parts[k - 1]
        for k in range(1, cols):
            col_copy(piece, (my_col + k) % cols).start()
        if piece < pieces - 1:
            gathered[piece, my_col] = parts[-1]
        else:
            lines[my_col] = parts[-1]

    for piece in everything:
        with jax.named_scope(f"colwait{piece}"):
            col_all(piece).wait_recv()
        if piece < pieces - 1:
            last_axis(gathered.at[piece], scale[piece % quads], wz, early.at[piece])
        if piece == pieces - 2:
            sent = send.at[:, pl.ds(0, rows - 1)]
            pltpu.make_async_copy(sent, sent, row_send).wait()
    sent = mixed.at[:, pl.ds(0, cols - 1)]
    pltpu.make_async_copy(sent, sent, col_send).wait()


def last_axis(lines, scale, wz, out):
    cols, half_y, _ = lines.shape
    width, _, nz = out.shape
    line = jnp.concatenate([lines[c] for c in range(cols)], axis=1)
    high, low = split(line)
    both = jnp.dot(jnp.concatenate([high, low], axis=0), wz[0], preferred_element_type=F32)
    done = both[:half_y] + both[half_y:]
    done = done + jnp.dot(high, wz[1], preferred_element_type=F32)
    done = done * scale
    for j in range(width):
        out[j] = done[:, j * padded(nz) : j * padded(nz) + nz]


def last_kernel(lines, scale, early, wz, out, held, out_sem):
    pieces = early.shape[0] + 1
    quads, width = scale.shape[0], held.shape[0]
    copies = []
    for piece in range(pieces):
        if piece == pieces - 1:
            last_axis(lines, scale[piece % quads], wz, held)
        source = early.at[piece] if piece < pieces - 1 else held
        place = out.at[piece // quads, pl.ds(piece % quads * width, width)]
        copy = pltpu.make_async_copy(source, place, out_sem.at[piece])
        copy.start()
        copies.append(copy)
    with jax.named_scope("outwait"):
        for copy in copies:
            copy.wait()


def on_device(rows, cols, species, symbol_x, symbol_y, symbol_z):
    fields, nx, share_y, share_z = species.shape
    ny, nz = symbol_y.shape[0], symbol_z.shape[0]
    share_x, half_y = nx // rows, ny // cols
    width = LANES // share_z
    quads = share_x // width
    pieces = fields * quads
    hx, hy, wz = (jnp.asarray(t) for t in tables(rows, nx, ny, nz, share_z))
    dma = pltpu.SemaphoreType.DMA
    regular = pltpu.SemaphoreType.REGULAR
    width_z = width * padded(nz)
    vmem = pl.BlockSpec(memory_space=pltpu.VMEM)
    lines, scale, early = pl.pallas_call(
        functools.partial(kernel, rows, cols, ("row", "col")),
        out_shape=(
            jax.ShapeDtypeStruct((cols, half_y, LANES), F32),
            jax.ShapeDtypeStruct((quads, half_y, width_z), F32),
            jax.ShapeDtypeStruct((pieces - 1, width, half_y, nz), F32),
        ),
        in_specs=[pl.BlockSpec(memory_space=pl.ANY)] * 7,
        out_specs=(vmem, vmem, vmem),
        scratch_shapes=[
            pltpu.VMEM((fields, nx // LANES, share_z, share_y, LANES), F32),
            pltpu.VMEM((fields, share_y * share_z, 2 * nx), F32),
            pltpu.VMEM(hx.shape, BF16),
            pltpu.VMEM(hy.shape, BF16),
            pltpu.VMEM(wz.shape, BF16),
            pltpu.VMEM((1, nx), F32),
            pltpu.VMEM((1, ny), F32),
            pltpu.VMEM((1, nz), F32),
            pltpu.VMEM((pieces, rows, share_y, LANES), F32),
            pltpu.VMEM((pieces, rows, share_y, LANES), F32),
            pltpu.VMEM((pieces, cols, half_y, LANES), F32),
            pltpu.VMEM((pieces - 1, cols, half_y, LANES), F32),
            pltpu.VMEM((nx, LANES), F32),
            pltpu.VMEM((ny, LANES), F32),
            dma((fields + 1,)),
            dma,
            dma((pieces,)),
            dma,
            dma((pieces,)),
            regular((2,)),
        ],
        compiler_params=pltpu.CompilerParams(collective_id=0, has_side_effects=True, vmem_limit_bytes=24 * 2**20),
    )(
        *(pltpu.with_memory_space_constraint(v, pltpu.HBM) for v in (jnp.transpose(species, (0, 2, 3, 1)), hx, hy,
        wz, symbol_x[None, :], symbol_y[None, :], symbol_z[None, :])),
    )
    return pl.pallas_call(
        last_kernel,
        out_shape=jax.ShapeDtypeStruct((fields, share_x, half_y, nz), F32),
        in_specs=[vmem, vmem, vmem, vmem],
        out_specs=pl.BlockSpec(memory_space=pl.ANY),
        scratch_shapes=[pltpu.VMEM((width, half_y, nz), F32), dma((pieces,))],
        compiler_params=pltpu.CompilerParams(vmem_limit_bytes=24 * 2**20),
    )(lines, scale, early, wz)


def solution(mesh):
    rows, cols = mesh.shape["row"], mesh.shape["col"]
    in_specs = (P(None, None, "row", "col"), P(), P(), P())
    out_specs = P(None, "row", "col", None)
    return jax.shard_map(
        functools.partial(on_device, rows, cols),
        mesh=mesh, in_specs=in_specs, out_specs=out_specs, check_vma=False,
    )
```

```python
import functools

import jax
import jax.numpy as jnp
import ml_dtypes
import numpy as np
from jax import lax
from jax.experimental import pallas as pl
from jax.experimental.pallas import tpu as pltpu
from jax.sharding import PartitionSpec as P

LANES = 128
GROUP = 4
F32, BF16 = jnp.float32, jnp.bfloat16
MESH = pl.DeviceIdType.MESH


def basis_table(count):
    odd = 2 * np.arange(count) + 1
    angle = np.pi / (4 * count) * (odd[:, None] * odd[None, :] % (8 * count))
    return np.cos(angle) * (2.0 / count) ** 0.5


def halves(table):
    high = table.astype(ml_dtypes.bfloat16)
    low = (table - high.astype(np.float64)).astype(ml_dtypes.bfloat16)
    return high, low


def split(values):
    high = values.astype(BF16)
    low = (values - high.astype(F32)).astype(BF16)
    return high, low


def padded(count):
    return -(-count // LANES) * LANES


def tables(rows, nx, ny, nz, share_z):
    width, half = LANES // share_z, share_z // 2
    share_x = nx // rows
    lane = np.arange(LANES)
    blocks = []
    for quad in range(share_x // width):
        for first in range(0, rows, half):
            column = lane[: LANES // 2]
            x = (first + column % half) * share_x + quad * width + column // half
            high, low = halves(basis_table(nx)[:, x])
            blocks += [high, low]
    table_x = np.tile(np.concatenate(blocks, axis=1), (2, 1))
    high, low = halves(basis_table(ny))
    table_y = np.block([[high, high], [low, low]])
    wide = np.zeros((nz // share_z, LANES, width, padded(nz)))
    for start in range(nz // share_z):
        z = start * share_z + lane % half + half * (lane // (LANES // 2))
        wide[start, lane, lane % (LANES // 2) // half, :nz] = basis_table(nz)[z]
    table_z = np.stack(halves(wide.reshape(-1, width * padded(nz))))
    return table_x, table_y, table_z


def kernel(
    rows, cols, names,
    species, hx_hbm, hy_hbm, wz_hbm, sx_hbm, sy_hbm, sz_hbm,
    lines, scale, early,
    xin, mid, hx, hy, wz, sx, sy, sz, send, recv, mixed, gathered, tall_x, tall_y,
    in_sem, row_send, row_recv, col_send, col_recv, row_ready,
):
    row_name, col_name = names
    fields, _, _, nx = species.shape
    ny, nz = sy.shape[1], sz.shape[1]
    share_y, share_z = ny // rows, nz // cols
    share_x, half_y = nx // rows, ny // cols
    width, half = LANES // share_z, share_z // 2
    quads = share_x // width
    pieces = fields * quads
    groups = rows // GROUP
    middle = groups // 2 - 1
    me, my_col = lax.axis_index(row_name), lax.axis_index(col_name)
    mine = me // GROUP

    def fetch(source, target, semaphore, parts):
        step = source.shape[0] // parts
        for i in range(parts):
            span = pl.ds(i * step, step)
            pltpu.make_async_copy(source.at[span], target.at[span], semaphore).start()

    blocks = nx // LANES
    def fetch_field(f):
        for b in range(blocks):
            for y in range(share_y):
                pltpu.make_async_copy(
                    species.at[f, y, :, pl.ds(b * LANES, LANES)], xin.at[f, b, :, y, :], in_sem.at[f]
                ).start()

    fetch(hx_hbm, hx, in_sem.at[0], 4)
    fetch_field(0)

    barrier = pltpu.get_barrier_semaphore()

    def greet_row(t, carry):
        pl.semaphore_signal(barrier, inc=1, device_id={row_name: t}, device_id_type=MESH)
        return carry

    def greet_col(t, carry):
        pl.semaphore_signal(barrier, inc=1, device_id={col_name: t}, device_id_type=MESH)
        return carry

    low = mine <= middle
    back = (mine - 1) * GROUP
    past = (mine > 0) & (mine <= middle + 1)
    first_half = me % GROUP < GROUP // 2
    back_from = back + jnp.where(first_half, 0, GROUP // 2)
    lax.fori_loop(jnp.where(past, back_from, 0), jnp.where(past, back + GROUP, 0), greet_row, 0)
    lax.fori_loop(me + 1, rows, greet_row, 0)
    lax.fori_loop(my_col + 1, cols, greet_col, 0)
    for f in range(1, fields):
        fetch_field(f)
    rest = ((hy_hbm, hy), (wz_hbm, wz), (sx_hbm, sx), (sy_hbm, sy), (sz_hbm, sz))
    fetches = [
        pltpu.make_async_copy(a, b, in_sem.at[fields]) for a, b in rest
    ]
    for copy in fetches:
        copy.start()

    def ready_row(t, carry):
        other = (~low & (t < (middle + 1) * GROUP)).astype(jnp.int32)
        other = jnp.where(past & (t >= back), jnp.where(t < back + GROUP, 2, other), other)
        pl.semaphore_signal(row_ready.at[other], inc=1, device_id={row_name: t}, device_id_type=MESH)
        return carry

    def ready_col(t, carry):
        pl.semaphore_signal(row_ready.at[0], inc=1, device_id={col_name: t}, device_id_type=MESH)
        return carry

    def meet():
        count = me + my_col + jnp.where(low, jnp.where(first_half, GROUP // 2, GROUP), 0)

        @pl.when(count > 0)
        def _():
            with jax.named_scope("barrier"):
                pl.semaphore_wait(barrier, count)

        lax.fori_loop(0, jnp.where(past, back_from, me), ready_row, 0)
        lax.fori_loop(jnp.where(past, mine * GROUP, me), me, ready_row, 0)
        lax.fori_loop(0, my_col, ready_col, 0)

    soon = (me % GROUP >= GROUP // 2) & ~low
    pl.when(soon)(meet)

    lane = lax.broadcasted_iota(jnp.int32, (share_y, LANES), 1)

    def row_copy(piece, target):
        return pltpu.make_async_remote_copy(
            src_ref=send.at[piece, target],
            dst_ref=recv.at[piece, me],
            send_sem=row_send,
            recv_sem=row_recv.at[piece],
            device_id={row_name: target},
            device_id_type=MESH,
        )

    def row_all(piece):
        return pltpu.make_async_remote_copy(
            src_ref=send.at[piece, pl.ds(0, rows - 1)],
            dst_ref=recv.at[piece, pl.ds(0, rows - 1)],
            send_sem=row_send,
            recv_sem=row_recv.at[piece],
            device_id={row_name: me},
            device_id_type=MESH,
        )

    def col_copy(piece, target):
        return pltpu.make_async_remote_copy(
            src_ref=mixed.at[piece, target],
            dst_ref=(gathered.at[piece, my_col] if piece < pieces - 1 else lines.at[my_col]),
            send_sem=col_send,
            recv_sem=col_recv.at[piece],
            device_id={col_name: target},
            device_id_type=MESH,
        )

    def col_all(piece):
        part = pl.ds(0, cols - 1)
        return pltpu.make_async_remote_copy(
            src_ref=mixed.at[piece, part],
            dst_ref=(gathered.at[piece, part] if piece < pieces - 1 else lines.at[part]),
            send_sem=col_send,
            recv_sem=col_recv.at[piece],
            device_id={col_name: my_col},
            device_id_type=MESH,
        )

    def send_to(least, most, some):
        for piece in some:

            def step(t, carry, piece=piece):
                row_copy(piece, t).start()
                return carry

            lax.fori_loop(least, most, step, 0)

    everything = range(pieces)
    front = jnp.minimum(mine, 1) * GROUP
    near_high = (mine + 2) * GROUP
    def product(f):
        cut = [
            split(xin[f, b].reshape(share_z * share_y, LANES)) for b in range(blocks)
        ]
        line = jnp.concatenate([part for pair in zip(*cut) for part in pair], axis=1)
        size = half * share_y
        for at in (0, size):
            mid[f, at : at + size] = jnp.dot(
                line[at : at + size], hx[...], preferred_element_type=F32
            )

    def load(f):
        pltpu.make_async_copy(xin.at[f], xin.at[f], in_sem.at[f]).wait()

    with jax.named_scope("load"):
        pltpu.make_async_copy(hx_hbm, hx, in_sem.at[0]).wait()
        load(0)
    product(0)
    for piece in everything:
        f, quad = piece // quads, piece % quads
        if quad == quads - 1 and f + 1 < fields:
            load(f + 1)
            product(f + 1)
        for block in range(rows // half):
            at = (quad * (rows // half) + block) * LANES
            tiles = [
                mid[f, z * share_y : (z + 1) * share_y, at : at + LANES] for z in range(share_z)
            ]
            keep = lane < LANES // 2
            tiles = [
                jnp.where(keep, a, b) + pltpu.roll(jnp.where(keep, b, a), LANES // 2, 1)
                for a, b in zip(tiles[:half], tiles[half:])
            ]
            unit = 1
            while unit < half:
                radix = min(4, half // unit)
                place = lane // unit % radix
                turned = list(tiles)
                for i in range(half):
                    own = i // unit % radix
                    for other in range(radix):
                        source = tiles[i + (other - own) * unit]
                        if other != own:
                            source = pltpu.roll(source, (other - own) * unit % LANES, 1)
                        turned[i] = source if other == 0 else jnp.where(place == other, source, turned[i])
                tiles = turned
                unit *= radix
            for i in range(half):
                send[piece, block * half + i] = tiles[i]
        if piece == 0:
            pl.when(~soon & ~low)(meet)
        with jax.named_scope(f"near{piece}"):

            @pl.when(~low)
            def _():
                send_to(0, front, [piece])

            if piece >= quads - 1:
                some = range(quads) if piece == quads - 1 else [piece]

                @pl.when(low)
                def _():
                    if piece == quads - 1:
                        meet()
                    for one in some:
                        send_to(0, front, [one])
                        send_to(near_high - GROUP, near_high - jnp.where(first_half, GROUP // 2, 0), [one])

            recv[piece, me] = send[piece, me]

    across = (jnp.where(mine > 0, GROUP, 0), jnp.minimum(mine, middle + 1) * GROUP)
    for f in range(fields):
        some = range(f * quads, (f + 1) * quads)
        for g in reversed(range(middle + 1, groups)):

            @pl.when(g < mine)
            def _():
                send_to(g * GROUP, (g + 1) * GROUP, some)

        send_to(*across, some)
    send_to(mine * GROUP, me, everything)

    @pl.when(low & first_half)
    def _():
        with jax.named_scope("ready2"):
            pl.semaphore_wait(row_ready.at[2], GROUP // 2)
        send_to(near_high - GROUP // 2, near_high, everything)

    half_end = jnp.where(low, (middle + 1) * GROUP, rows)
    last = jnp.minimum((mine + 1) * GROUP, half_end)
    greeted = jnp.where(low, jnp.minimum((mine + 2) * GROUP, half_end), last)
    count = half_end - me - 1 - (greeted - last) + cols - 1 - my_col

    @pl.when(count > 0)
    def _():
        with jax.named_scope("ready0"):
            pl.semaphore_wait(row_ready.at[0], count)

    send_to(me + 1, last, everything)
    send_to(greeted, half_end, everything)

    @pl.when(low)
    def _():
        far = jnp.maximum(mine + 2, middle + 1) * GROUP
        with jax.named_scope("ready1"):
            pl.semaphore_wait(row_ready.at[1], rows - far)
        send_to(far, rows, everything)

    for copy in fetches:
        copy.wait()
    tall_x[...] = jnp.broadcast_to(sx[...], (LANES, nx)).T
    tall_y[...] = jnp.broadcast_to(sy[...], (LANES, ny)).T
    part_y = tall_y[pl.ds(my_col * half_y, half_y), :1]
    for x in range(share_x):
        part_x = tall_x[pl.ds(me * share_x + x, 1), :1]
        at = x % width * padded(nz)
        scale[x // width, :, at : at + nz] = 1.0 / (part_x + part_y + sz[...])

    for piece in everything:
        with jax.named_scope(f"rowwait{piece}"):
            row_all(piece).wait_recv()
        high, low = split(recv[piece].reshape(ny, LANES))
        stacked = jnp.concatenate([high, low], axis=0)
        parts = []
        for k in range(1, cols + 1):
            at = pl.multiple_of((my_col + k) % cols * half_y, half_y)
            table = jnp.concatenate([hy[pl.ds(at, half_y), :], hy[pl.ds(ny + at, half_y), :]], axis=0)
            both = jnp.dot(table, stacked, preferred_element_type=F32)
            parts.append(both[:half_y] + both[half_y:])
        for k in range(1, cols):
            mixed[piece, (my_col + k) % cols] = parts[k - 1]
        for k in range(1, cols):
            col_copy(piece, (my_col + k) % cols).start()
        if piece < pieces - 1:
            gathered[piece, my_col] = parts[-1]
        else:
            lines[my_col] = parts[-1]

    for piece in everything:
        with jax.named_scope(f"colwait{piece}"):
            col_all(piece).wait_recv()
        if piece < pieces - 1:
            last_axis(gathered.at[piece], scale[piece % quads], wz, early.at[piece])
        if piece == pieces - 2:
            sent = send.at[:, pl.ds(0, rows - 1)]
            pltpu.make_async_copy(sent, sent, row_send).wait()
    sent = mixed.at[:, pl.ds(0, cols - 1)]
    pltpu.make_async_copy(sent, sent, col_send).wait()


def last_axis(lines, scale, wz, out):
    cols, half_y, _ = lines.shape
    width, _, nz = out.shape
    line = jnp.concatenate([lines[c] for c in range(cols)], axis=1)
    high, low = split(line)
    both = jnp.dot(jnp.concatenate([high, low], axis=0), wz[0], preferred_element_type=F32)
    done = both[:half_y] + both[half_y:]
    done = done + jnp.dot(high, wz[1], preferred_element_type=F32)
    done = done * scale
    for j in range(width):
        out[j] = done[:, j * padded(nz) : j * padded(nz) + nz]


def last_kernel(lines, scale, early, wz, out, held, out_sem):
    pieces = early.shape[0] + 1
    quads, width = scale.shape[0], held.shape[0]
    copies = []
    for piece in range(pieces):
        if piece == pieces - 1:
            last_axis(lines, scale[piece % quads], wz, held)
        source = early.at[piece] if piece < pieces - 1 else held
        place = out.at[piece // quads, pl.ds(piece % quads * width, width)]
        copy = pltpu.make_async_copy(source, place, out_sem.at[piece])
        copy.start()
        copies.append(copy)
    with jax.named_scope("outwait"):
        for copy in copies:
            copy.wait()


def on_device(rows, cols, species, symbol_x, symbol_y, symbol_z):
    fields, nx, share_y, share_z = species.shape
    ny, nz = symbol_y.shape[0], symbol_z.shape[0]
    share_x, half_y = nx // rows, ny // cols
    width = LANES // share_z
    quads = share_x // width
    pieces = fields * quads
    hx, hy, wz = (jnp.asarray(t) for t in tables(rows, nx, ny, nz, share_z))
    dma = pltpu.SemaphoreType.DMA
    regular = pltpu.SemaphoreType.REGULAR
    width_z = width * padded(nz)
    vmem = pl.BlockSpec(memory_space=pltpu.VMEM)
    lines, scale, early = pl.pallas_call(
        functools.partial(kernel, rows, cols, ("row", "col")),
        out_shape=(
            jax.ShapeDtypeStruct((cols, half_y, LANES), F32),
            jax.ShapeDtypeStruct((quads, half_y, width_z), F32),
            jax.ShapeDtypeStruct((pieces - 1, width, half_y, nz), F32),
        ),
        in_specs=[pl.BlockSpec(memory_space=pl.ANY)] * 7,
        out_specs=(vmem, vmem, vmem),
        scratch_shapes=[
            pltpu.VMEM((fields, nx // LANES, share_z, share_y, LANES), F32),
            pltpu.VMEM((fields, share_y * share_z, 2 * nx), F32),
            pltpu.VMEM(hx.shape, BF16),
            pltpu.VMEM(hy.shape, BF16),
            pltpu.VMEM(wz.shape, BF16),
            pltpu.VMEM((1, nx), F32),
            pltpu.VMEM((1, ny), F32),
            pltpu.VMEM((1, nz), F32),
            pltpu.VMEM((pieces, rows, share_y, LANES), F32),
            pltpu.VMEM((pieces, rows, share_y, LANES), F32),
            pltpu.VMEM((pieces, cols, half_y, LANES), F32),
            pltpu.VMEM((pieces - 1, cols, half_y, LANES), F32),
            pltpu.VMEM((nx, LANES), F32),
            pltpu.VMEM((ny, LANES), F32),
            dma((fields + 1,)),
            dma,
            dma((pieces,)),
            dma,
            dma((pieces,)),
            regular((3,)),
        ],
        compiler_params=pltpu.CompilerParams(collective_id=0, has_side_effects=True, vmem_limit_bytes=24 * 2**20),
    )(
        *(pltpu.with_memory_space_constraint(v, pltpu.HBM) for v in (jnp.transpose(species, (0, 2, 3, 1)), hx, hy,
        wz, symbol_x[None, :], symbol_y[None, :], symbol_z[None, :])),
    )
    return pl.pallas_call(
        last_kernel,
        out_shape=jax.ShapeDtypeStruct((fields, share_x, half_y, nz), F32),
        in_specs=[vmem, vmem, vmem, vmem],
        out_specs=pl.BlockSpec(memory_space=pl.ANY),
        scratch_shapes=[pltpu.VMEM((width, half_y, nz), F32), dma((pieces,))],
        compiler_params=pltpu.CompilerParams(vmem_limit_bytes=24 * 2**20),
    )(lines, scale, early, wz)


def solution(mesh):
    rows, cols = mesh.shape["row"], mesh.shape["col"]
    in_specs = (P(None, None, "row", "col"), P(), P(), P())
    out_specs = P(None, "row", "col", None)
    return jax.shard_map(
        functools.partial(on_device, rows, cols),
        mesh=mesh, in_specs=in_specs, out_specs=out_specs, check_vma=False,
    )
```

```python
import functools

import jax
import jax.numpy as jnp
import ml_dtypes
import numpy as np
from jax import lax
from jax.experimental import pallas as pl
from jax.experimental.pallas import tpu as pltpu
from jax.sharding import PartitionSpec as P

LANES = 128
GROUP = 4
F32, BF16 = jnp.float32, jnp.bfloat16
MESH = pl.DeviceIdType.MESH


def basis_table(count):
    odd = 2 * np.arange(count) + 1
    angle = np.pi / (4 * count) * (odd[:, None] * odd[None, :] % (8 * count))
    return np.cos(angle) * (2.0 / count) ** 0.5


def halves(table):
    high = table.astype(ml_dtypes.bfloat16)
    low = (table - high.astype(np.float64)).astype(ml_dtypes.bfloat16)
    return high, low


def split(values):
    high = values.astype(BF16)
    low = (values - high.astype(F32)).astype(BF16)
    return high, low


def padded(count):
    return -(-count // LANES) * LANES


def tables(rows, nx, ny, nz, share_z):
    width, half = LANES // share_z, share_z // 2
    share_x = nx // rows
    lane = np.arange(LANES)
    blocks = []
    for quad in range(share_x // width):
        for first in range(0, rows, half):
            column = lane[: LANES // 2]
            x = (first + column % half) * share_x + quad * width + column // half
            high, low = halves(basis_table(nx)[:, x])
            blocks += [high, low]
    table_x = np.tile(np.concatenate(blocks, axis=1), (2, 1))
    high, low = halves(basis_table(ny))
    table_y = np.block([[high, high], [low, low]])
    wide = np.zeros((nz // share_z, LANES, width, padded(nz)))
    for start in range(nz // share_z):
        z = start * share_z + lane % half + half * (lane // (LANES // 2))
        wide[start, lane, lane % (LANES // 2) // half, :nz] = basis_table(nz)[z]
    table_z = np.stack(halves(wide.reshape(-1, width * padded(nz))))
    return table_x, table_y, table_z


def kernel(
    rows, cols, names,
    species, hx_hbm, hy_hbm, wz_hbm, sx_hbm, sy_hbm, sz_hbm,
    lines, scale, early,
    xin, mid, hx, hy, wz, sx, sy, sz, send, recv, mixed, gathered, tall_x, tall_y,
    in_sem, row_send, row_recv, col_send, col_recv, row_ready,
):
    row_name, col_name = names
    fields, _, _, nx = species.shape
    ny, nz = sy.shape[1], sz.shape[1]
    share_y, share_z = ny // rows, nz // cols
    share_x, half_y = nx // rows, ny // cols
    width, half = LANES // share_z, share_z // 2
    quads = share_x // width
    pieces = fields * quads
    groups = rows // GROUP
    middle = groups // 2 - 1
    me, my_col = lax.axis_index(row_name), lax.axis_index(col_name)
    mine = me // GROUP

    def fetch(source, target, semaphore, parts):
        step = source.shape[0] // parts
        for i in range(parts):
            span = pl.ds(i * step, step)
            pltpu.make_async_copy(source.at[span], target.at[span], semaphore).start()

    blocks = nx // LANES
    def fetch_field(f):
        for b in range(blocks):
            for y in range(share_y):
                pltpu.make_async_copy(
                    species.at[f, y, :, pl.ds(b * LANES, LANES)], xin.at[f, b, :, y, :], in_sem.at[f]
                ).start()

    fetch(hx_hbm, hx, in_sem.at[0], 4)
    fetch_field(0)

    barrier = pltpu.get_barrier_semaphore()

    def greet_row(t, carry):
        pl.semaphore_signal(barrier, inc=1, device_id={row_name: t}, device_id_type=MESH)
        return carry

    def greet_col(t, carry):
        pl.semaphore_signal(barrier, inc=1, device_id={col_name: t}, device_id_type=MESH)
        return carry

    low = mine <= middle
    back = (mine - 1) * GROUP
    past = (mine > 0) & (mine <= middle + 1)
    first_half = me % GROUP < GROUP // 2
    back_from = back + jnp.where(first_half, 0, GROUP // 2)
    lax.fori_loop(jnp.where(past, back_from, 0), jnp.where(past, back + GROUP, 0), greet_row, 0)
    lax.fori_loop(me + 1, rows, greet_row, 0)
    lax.fori_loop(my_col + 1, cols, greet_col, 0)
    for f in range(1, fields):
        fetch_field(f)
    rest = ((hy_hbm, hy), (wz_hbm, wz), (sx_hbm, sx), (sy_hbm, sy), (sz_hbm, sz))
    fetches = [
        pltpu.make_async_copy(a, b, in_sem.at[fields]) for a, b in rest
    ]
    for copy in fetches:
        copy.start()

    def ready_row(t, carry):
        other = (~low & (t < (middle + 1) * GROUP)).astype(jnp.int32)
        other = jnp.where(past & (t >= back), jnp.where(t < back + GROUP, 2, other), other)
        pl.semaphore_signal(row_ready.at[other], inc=1, device_id={row_name: t}, device_id_type=MESH)
        return carry

    def ready_col(t, carry):
        pl.semaphore_signal(row_ready.at[0], inc=1, device_id={col_name: t}, device_id_type=MESH)
        return carry

    def meet():
        count = me + my_col + jnp.where(low, jnp.where(first_half, GROUP // 2, GROUP), 0)

        @pl.when(count > 0)
        def _():
            with jax.named_scope("barrier"):
                pl.semaphore_wait(barrier, count)

        lax.fori_loop(0, jnp.where(past, back_from, me), ready_row, 0)
        lax.fori_loop(jnp.where(past, mine * GROUP, me), me, ready_row, 0)
        lax.fori_loop(0, my_col, ready_col, 0)

    soon = (me % GROUP >= GROUP // 2) & ~low
    pl.when(soon)(meet)

    lane = lax.broadcasted_iota(jnp.int32, (share_y, LANES), 1)

    def row_copy(piece, target):
        return pltpu.make_async_remote_copy(
            src_ref=send.at[piece, target],
            dst_ref=recv.at[piece, me],
            send_sem=row_send,
            recv_sem=row_recv.at[piece],
            device_id={row_name: target},
            device_id_type=MESH,
        )

    def row_all(piece):
        return pltpu.make_async_remote_copy(
            src_ref=send.at[piece, pl.ds(0, rows - 1)],
            dst_ref=recv.at[piece, pl.ds(0, rows - 1)],
            send_sem=row_send,
            recv_sem=row_recv.at[piece],
            device_id={row_name: me},
            device_id_type=MESH,
        )

    def col_copy(piece, target):
        return pltpu.make_async_remote_copy(
            src_ref=mixed.at[piece, target],
            dst_ref=(gathered.at[piece, my_col] if piece < pieces - 1 else lines.at[my_col]),
            send_sem=col_send,
            recv_sem=col_recv.at[piece],
            device_id={col_name: target},
            device_id_type=MESH,
        )

    def col_all(piece):
        part = pl.ds(0, cols - 1)
        return pltpu.make_async_remote_copy(
            src_ref=mixed.at[piece, part],
            dst_ref=(gathered.at[piece, part] if piece < pieces - 1 else lines.at[part]),
            send_sem=col_send,
            recv_sem=col_recv.at[piece],
            device_id={col_name: my_col},
            device_id_type=MESH,
        )

    def send_to(least, most, some):
        for piece in some:

            def step(t, carry, piece=piece):
                row_copy(piece, t).start()
                return carry

            lax.fori_loop(least, most, step, 0)

    everything = range(pieces)
    front = jnp.minimum(mine, 1) * (GROUP // 2)
    near_high = (mine + 2) * GROUP
    def product(f):
        cut = [
            split(xin[f, b].reshape(share_z * share_y, LANES)) for b in range(blocks)
        ]
        line = jnp.concatenate([part for pair in zip(*cut) for part in pair], axis=1)
        size = half * share_y
        for at in (0, size):
            mid[f, at : at + size] = jnp.dot(
                line[at : at + size], hx[...], preferred_element_type=F32
            )

    def load(f):
        pltpu.make_async_copy(xin.at[f], xin.at[f], in_sem.at[f]).wait()

    with jax.named_scope("load"):
        pltpu.make_async_copy(hx_hbm, hx, in_sem.at[0]).wait()
        load(0)
    product(0)
    for piece in everything:
        f, quad = piece // quads, piece % quads
        if quad == quads - 1 and f + 1 < fields:
            load(f + 1)
            product(f + 1)
        for block in range(rows // half):
            at = (quad * (rows // half) + block) * LANES
            tiles = [
                mid[f, z * share_y : (z + 1) * share_y, at : at + LANES] for z in range(share_z)
            ]
            keep = lane < LANES // 2
            tiles = [
                jnp.where(keep, a, b) + pltpu.roll(jnp.where(keep, b, a), LANES // 2, 1)
                for a, b in zip(tiles[:half], tiles[half:])
            ]
            unit = 1
            while unit < half:
                radix = min(4, half // unit)
                place = lane // unit % radix
                turned = list(tiles)
                for i in range(half):
                    own = i // unit % radix
                    for other in range(radix):
                        source = tiles[i + (other - own) * unit]
                        if other != own:
                            source = pltpu.roll(source, (other - own) * unit % LANES, 1)
                        turned[i] = source if other == 0 else jnp.where(place == other, source, turned[i])
                tiles = turned
                unit *= radix
            for i in range(half):
                send[piece, block * half + i] = tiles[i]
        if piece == 0:
            pl.when(~soon & ~low)(meet)
        with jax.named_scope(f"near{piece}"):

            @pl.when(~low)
            def _():
                send_to(0, front, [piece])

            if piece >= quads - 1:
                some = range(quads) if piece == quads - 1 else [piece]

                @pl.when(low)
                def _():
                    if piece == quads - 1:
                        meet()
                    for one in some:
                        send_to(0, front, [one])
                        send_to(near_high - GROUP, near_high - jnp.where(first_half, GROUP // 2, 0), [one])

            recv[piece, me] = send[piece, me]

    across = (jnp.where(mine > 0, GROUP, 0), jnp.minimum(mine, middle + 1) * GROUP)

    def send_near(some):
        for g in reversed(range(middle + 1, groups)):

            @pl.when(g < mine)
            def _():
                send_to(g * GROUP, (g + 1) * GROUP, some)

    for f in range(fields):
        some = range(f * quads, (f + 1) * quads)
        send_to(front, 2 * front, some)
        send_near(some)
        send_to(*across, some)
    send_to(mine * GROUP, me, everything)

    @pl.when(low & first_half)
    def _():
        with jax.named_scope("ready2"):
            pl.semaphore_wait(row_ready.at[2], GROUP // 2)
        send_to(near_high - GROUP // 2, near_high, everything)

    half_end = jnp.where(low, (middle + 1) * GROUP, rows)
    last = jnp.minimum((mine + 1) * GROUP, half_end)
    greeted = jnp.where(low, jnp.minimum((mine + 2) * GROUP, half_end), last)
    count = half_end - me - 1 - (greeted - last) + cols - 1 - my_col

    @pl.when(count > 0)
    def _():
        with jax.named_scope("ready0"):
            pl.semaphore_wait(row_ready.at[0], count)

    send_to(me + 1, last, everything)
    send_to(greeted, half_end, everything)

    @pl.when(low)
    def _():
        far = jnp.maximum(mine + 2, middle + 1) * GROUP
        with jax.named_scope("ready1"):
            pl.semaphore_wait(row_ready.at[1], rows - far)
        send_to(far, rows, everything)

    for copy in fetches:
        copy.wait()
    tall_x[...] = jnp.broadcast_to(sx[...], (LANES, nx)).T
    tall_y[...] = jnp.broadcast_to(sy[...], (LANES, ny)).T
    part_y = tall_y[pl.ds(my_col * half_y, half_y), :1]
    for x in range(share_x):
        part_x = tall_x[pl.ds(me * share_x + x, 1), :1]
        at = x % width * padded(nz)
        scale[x // width, :, at : at + nz] = 1.0 / (part_x + part_y + sz[...])

    for piece in everything:
        with jax.named_scope(f"rowwait{piece}"):
            row_all(piece).wait_recv()
        high, low = split(recv[piece].reshape(ny, LANES))
        stacked = jnp.concatenate([high, low], axis=0)
        parts = []
        for k in range(1, cols + 1):
            at = pl.multiple_of((my_col + k) % cols * half_y, half_y)
            table = jnp.concatenate([hy[pl.ds(at, half_y), :], hy[pl.ds(ny + at, half_y), :]], axis=0)
            both = jnp.dot(table, stacked, preferred_element_type=F32)
            parts.append(both[:half_y] + both[half_y:])
        for k in range(1, cols):
            mixed[piece, (my_col + k) % cols] = parts[k - 1]
        for k in range(1, cols):
            col_copy(piece, (my_col + k) % cols).start()
        if piece < pieces - 1:
            gathered[piece, my_col] = parts[-1]
        else:
            lines[my_col] = parts[-1]

    for piece in everything:
        with jax.named_scope(f"colwait{piece}"):
            col_all(piece).wait_recv()
        if piece < pieces - 1:
            last_axis(gathered.at[piece], scale[piece % quads], wz, early.at[piece])
        if piece == pieces - 2:
            sent = send.at[:, pl.ds(0, rows - 1)]
            pltpu.make_async_copy(sent, sent, row_send).wait()
    sent = mixed.at[:, pl.ds(0, cols - 1)]
    pltpu.make_async_copy(sent, sent, col_send).wait()


def last_axis(lines, scale, wz, out):
    cols, half_y, _ = lines.shape
    width, _, nz = out.shape
    line = jnp.concatenate([lines[c] for c in range(cols)], axis=1)
    high, low = split(line)
    both = jnp.dot(jnp.concatenate([high, low], axis=0), wz[0], preferred_element_type=F32)
    done = both[:half_y] + both[half_y:]
    done = done + jnp.dot(high, wz[1], preferred_element_type=F32)
    done = done * scale
    for j in range(width):
        out[j] = done[:, j * padded(nz) : j * padded(nz) + nz]


def last_kernel(lines, scale, early, wz, out, held, out_sem):
    pieces = early.shape[0] + 1
    quads, width = scale.shape[0], held.shape[0]
    copies = []
    for piece in range(pieces):
        if piece == pieces - 1:
            last_axis(lines, scale[piece % quads], wz, held)
        source = early.at[piece] if piece < pieces - 1 else held
        place = out.at[piece // quads, pl.ds(piece % quads * width, width)]
        copy = pltpu.make_async_copy(source, place, out_sem.at[piece])
        copy.start()
        copies.append(copy)
    with jax.named_scope("outwait"):
        for copy in copies:
            copy.wait()


def on_device(rows, cols, species, symbol_x, symbol_y, symbol_z):
    fields, nx, share_y, share_z = species.shape
    ny, nz = symbol_y.shape[0], symbol_z.shape[0]
    share_x, half_y = nx // rows, ny // cols
    width = LANES // share_z
    quads = share_x // width
    pieces = fields * quads
    hx, hy, wz = (jnp.asarray(t) for t in tables(rows, nx, ny, nz, share_z))
    dma = pltpu.SemaphoreType.DMA
    regular = pltpu.SemaphoreType.REGULAR
    width_z = width * padded(nz)
    vmem = pl.BlockSpec(memory_space=pltpu.VMEM)
    lines, scale, early = pl.pallas_call(
        functools.partial(kernel, rows, cols, ("row", "col")),
        out_shape=(
            jax.ShapeDtypeStruct((cols, half_y, LANES), F32),
            jax.ShapeDtypeStruct((quads, half_y, width_z), F32),
            jax.ShapeDtypeStruct((pieces - 1, width, half_y, nz), F32),
        ),
        in_specs=[pl.BlockSpec(memory_space=pl.ANY)] * 7,
        out_specs=(vmem, vmem, vmem),
        scratch_shapes=[
            pltpu.VMEM((fields, nx // LANES, share_z, share_y, LANES), F32),
            pltpu.VMEM((fields, share_y * share_z, 2 * nx), F32),
            pltpu.VMEM(hx.shape, BF16),
            pltpu.VMEM(hy.shape, BF16),
            pltpu.VMEM(wz.shape, BF16),
            pltpu.VMEM((1, nx), F32),
            pltpu.VMEM((1, ny), F32),
            pltpu.VMEM((1, nz), F32),
            pltpu.VMEM((pieces, rows, share_y, LANES), F32),
            pltpu.VMEM((pieces, rows, share_y, LANES), F32),
            pltpu.VMEM((pieces, cols, half_y, LANES), F32),
            pltpu.VMEM((pieces - 1, cols, half_y, LANES), F32),
            pltpu.VMEM((nx, LANES), F32),
            pltpu.VMEM((ny, LANES), F32),
            dma((fields + 1,)),
            dma,
            dma((pieces,)),
            dma,
            dma((pieces,)),
            regular((3,)),
        ],
        compiler_params=pltpu.CompilerParams(collective_id=0, has_side_effects=True, vmem_limit_bytes=24 * 2**20),
    )(
        *(pltpu.with_memory_space_constraint(v, pltpu.HBM) for v in (jnp.transpose(species, (0, 2, 3, 1)), hx, hy,
        wz, symbol_x[None, :], symbol_y[None, :], symbol_z[None, :])),
    )
    return pl.pallas_call(
        last_kernel,
        out_shape=jax.ShapeDtypeStruct((fields, share_x, half_y, nz), F32),
        in_specs=[vmem, vmem, vmem, vmem],
        out_specs=pl.BlockSpec(memory_space=pl.ANY),
        scratch_shapes=[pltpu.VMEM((width, half_y, nz), F32), dma((pieces,))],
        compiler_params=pltpu.CompilerParams(vmem_limit_bytes=24 * 2**20),
    )(lines, scale, early, wz)


def solution(mesh):
    rows, cols = mesh.shape["row"], mesh.shape["col"]
    in_specs = (P(None, None, "row", "col"), P(), P(), P())
    out_specs = P(None, "row", "col", None)
    return jax.shard_map(
        functools.partial(on_device, rows, cols),
        mesh=mesh, in_specs=in_specs, out_specs=out_specs, check_vma=False,
    )
```

```python
import functools

import jax
import jax.numpy as jnp
import ml_dtypes
import numpy as np
from jax import lax
from jax.experimental import pallas as pl
from jax.experimental.pallas import tpu as pltpu
from jax.sharding import PartitionSpec as P

LANES = 128
GROUP = 4
F32, BF16 = jnp.float32, jnp.bfloat16
MESH = pl.DeviceIdType.MESH


def basis_table(count):
    odd = 2 * np.arange(count) + 1
    angle = np.pi / (4 * count) * (odd[:, None] * odd[None, :] % (8 * count))
    return np.cos(angle) * (2.0 / count) ** 0.5


def halves(table):
    high = table.astype(ml_dtypes.bfloat16)
    low = (table - high.astype(np.float64)).astype(ml_dtypes.bfloat16)
    return high, low


def split(values):
    high = values.astype(BF16)
    low = (values - high.astype(F32)).astype(BF16)
    return high, low


def padded(count):
    return -(-count // LANES) * LANES


def tables(rows, nx, ny, nz, share_z):
    width, half = LANES // share_z, share_z // 2
    share_x = nx // rows
    lane = np.arange(LANES)
    blocks = []
    for quad in range(share_x // width):
        for first in range(0, rows, half):
            column = lane[: LANES // 2]
            x = (first + column % half) * share_x + quad * width + column // half
            high, low = halves(basis_table(nx)[:, x])
            blocks += [high, low]
    table_x = np.tile(np.concatenate(blocks, axis=1), (2, 1))
    high, low = halves(basis_table(ny))
    table_y = np.block([[high, high], [low, low]])
    wide = np.zeros((nz // share_z, LANES, width, padded(nz)))
    for start in range(nz // share_z):
        z = start * share_z + lane % half + half * (lane // (LANES // 2))
        wide[start, lane, lane % (LANES // 2) // half, :nz] = basis_table(nz)[z]
    table_z = np.stack(halves(wide.reshape(-1, width * padded(nz))))
    return table_x, table_y, table_z


def kernel(
    rows, cols, names,
    species, hx_hbm, hy_hbm, wz_hbm, sx_hbm, sy_hbm, sz_hbm,
    lines, scale, early,
    xin, mid, hx, hy, wz, sx, sy, sz, send, recv, mixed, gathered, tall_x, tall_y,
    row_send, row_recv, col_send, col_recv, row_ready,
):
    row_name, col_name = names
    fields, _, _, nx = species.shape
    ny, nz = sy.shape[1], sz.shape[1]
    share_y, share_z = ny // rows, nz // cols
    share_x, half_y = nx // rows, ny // cols
    width, half = LANES // share_z, share_z // 2
    quads = share_x // width
    pieces = fields * quads
    groups = rows // GROUP
    middle = groups // 2 - 1
    me, my_col = lax.axis_index(row_name), lax.axis_index(col_name)
    mine = me // GROUP

    def fetch(source, target, semaphore, parts):
        step = source.shape[0] // parts
        for i in range(parts):
            span = pl.ds(i * step, step)
            pltpu.make_async_copy(source.at[span], target.at[span], semaphore).start()

    blocks = nx // LANES
    landed = (row_send, *([col_send] * (fields - 1)))

    def fetch_field(f):
        for b in range(blocks):
            for y in range(share_y):
                pltpu.make_async_copy(
                    species.at[f, y, :, pl.ds(b * LANES, LANES)], xin.at[f, b, :, y, :], landed[f]
                ).start()

    fetch(hx_hbm, hx, row_send, 4)
    fetch_field(0)

    barrier = pltpu.get_barrier_semaphore()

    def greet_row(t, carry):
        pl.semaphore_signal(barrier, inc=1, device_id={row_name: t}, device_id_type=MESH)
        return carry

    def greet_col(t, carry):
        pl.semaphore_signal(barrier, inc=1, device_id={col_name: t}, device_id_type=MESH)
        return carry

    low = mine <= middle
    back = (mine - 1) * GROUP
    past = (mine > 0) & (mine <= middle + 1)
    first_half = me % GROUP < GROUP // 2
    back_from = back + jnp.where(first_half, 0, GROUP // 2)
    lax.fori_loop(jnp.where(past, back_from, 0), jnp.where(past, back + GROUP, 0), greet_row, 0)
    lax.fori_loop(me + 1, rows, greet_row, 0)
    lax.fori_loop(my_col + 1, cols, greet_col, 0)
    for f in range(1, fields):
        fetch_field(f)
    rest = ((hy_hbm, hy), (wz_hbm, wz), (sx_hbm, sx), (sy_hbm, sy), (sz_hbm, sz))
    fetches = [pltpu.make_async_copy(a, b, col_send) for a, b in rest]

    def ready_row(t, carry):
        other = (~low & (t < (middle + 1) * GROUP)).astype(jnp.int32)
        other = jnp.where(past & (t >= back), jnp.where(t < back + GROUP, 2, other), other)
        pl.semaphore_signal(row_ready.at[other], inc=1, device_id={row_name: t}, device_id_type=MESH)
        return carry

    def ready_col(t, carry):
        pl.semaphore_signal(row_ready.at[0], inc=1, device_id={col_name: t}, device_id_type=MESH)
        return carry

    def meet():
        count = me + my_col + jnp.where(low, jnp.where(first_half, GROUP // 2, GROUP), 0)

        @pl.when(count > 0)
        def _():
            with jax.named_scope("barrier"):
                pl.semaphore_wait(barrier, count)

        lax.fori_loop(0, jnp.where(past, back_from, me), ready_row, 0)
        lax.fori_loop(jnp.where(past, mine * GROUP, me), me, ready_row, 0)
        lax.fori_loop(0, my_col, ready_col, 0)

    soon = (me % GROUP >= GROUP // 2) & ~low
    pl.when(soon)(meet)

    lane = lax.broadcasted_iota(jnp.int32, (share_y, LANES), 1)

    def row_copy(piece, target):
        return pltpu.make_async_remote_copy(
            src_ref=send.at[piece, target],
            dst_ref=recv.at[piece, me],
            send_sem=row_send,
            recv_sem=row_recv.at[piece],
            device_id={row_name: target},
            device_id_type=MESH,
        )

    def row_all(piece):
        return pltpu.make_async_remote_copy(
            src_ref=send.at[piece, pl.ds(0, rows - 1)],
            dst_ref=recv.at[piece, pl.ds(0, rows - 1)],
            send_sem=row_send,
            recv_sem=row_recv.at[piece],
            device_id={row_name: me},
            device_id_type=MESH,
        )

    def col_copy(piece, target):
        return pltpu.make_async_remote_copy(
            src_ref=mixed.at[piece, target],
            dst_ref=(gathered.at[piece, my_col] if piece < pieces - 1 else lines.at[my_col]),
            send_sem=col_send,
            recv_sem=col_recv.at[piece],
            device_id={col_name: target},
            device_id_type=MESH,
        )

    def col_all(piece):
        part = pl.ds(0, cols - 1)
        return pltpu.make_async_remote_copy(
            src_ref=mixed.at[piece, part],
            dst_ref=(gathered.at[piece, part] if piece < pieces - 1 else lines.at[part]),
            send_sem=col_send,
            recv_sem=col_recv.at[piece],
            device_id={col_name: my_col},
            device_id_type=MESH,
        )

    def send_to(least, most, some):
        for piece in some:

            def step(t, carry, piece=piece):
                row_copy(piece, t).start()
                return carry

            lax.fori_loop(least, most, step, 0)

    everything = range(pieces)
    front = jnp.minimum(mine, 1) * (GROUP // 2)
    near_high = (mine + 2) * GROUP
    def product(f):
        cut = [
            split(xin[f, b].reshape(share_z * share_y, LANES)) for b in range(blocks)
        ]
        line = jnp.concatenate([part for pair in zip(*cut) for part in pair], axis=1)
        size = half * share_y
        for at in (0, size):
            mid[f, at : at + size] = jnp.dot(
                line[at : at + size], hx[...], preferred_element_type=F32
            )

    def load(f):
        pltpu.make_async_copy(xin.at[f], xin.at[f], landed[f]).wait()

    with jax.named_scope("load"):
        pltpu.make_async_copy(hx_hbm, hx, row_send).wait()
        load(0)
    product(0)
    for piece in everything:
        f, quad = piece // quads, piece % quads
        if quad == quads - 1 and f + 1 < fields:
            load(f + 1)
            product(f + 1)
            if f + 2 == fields:
                for copy in fetches:
                    copy.start()
        for block in range(rows // half):
            at = (quad * (rows // half) + block) * LANES
            tiles = [
                mid[f, z * share_y : (z + 1) * share_y, at : at + LANES] for z in range(share_z)
            ]
            keep = lane < LANES // 2
            tiles = [
                jnp.where(keep, a, b) + pltpu.roll(jnp.where(keep, b, a), LANES // 2, 1)
                for a, b in zip(tiles[:half], tiles[half:])
            ]
            unit = 1
            while unit < half:
                radix = min(4, half // unit)
                place = lane // unit % radix
                turned = list(tiles)
                for i in range(half):
                    own = i // unit % radix
                    for other in range(radix):
                        source = tiles[i + (other - own) * unit]
                        if other != own:
                            source = pltpu.roll(source, (other - own) * unit % LANES, 1)
                        turned[i] = source if other == 0 else jnp.where(place == other, source, turned[i])
                tiles = turned
                unit *= radix
            for i in range(half):
                send[piece, block * half + i] = tiles[i]
        if piece == 0:
            pl.when(~soon & ~low)(meet)
        with jax.named_scope(f"near{piece}"):

            @pl.when(~low)
            def _():
                send_to(0, front, [piece])

            if piece >= quads - 1:
                some = range(quads) if piece == quads - 1 else [piece]

                @pl.when(low)
                def _():
                    if piece == quads - 1:
                        meet()
                    for one in some:
                        send_to(0, front, [one])
                        send_to(near_high - GROUP, near_high - jnp.where(first_half, GROUP // 2, 0), [one])

            recv[piece, me] = send[piece, me]

    across = (jnp.where(mine > 0, GROUP, 0), jnp.minimum(mine, middle + 1) * GROUP)

    def send_near(some):
        for g in reversed(range(middle + 1, groups)):

            @pl.when(g < mine)
            def _():
                send_to(g * GROUP, (g + 1) * GROUP, some)

    for f in range(fields):
        some = range(f * quads, (f + 1) * quads)
        send_to(front, 2 * front, some)
        send_near(some)
        send_to(*across, some)
    send_to(mine * GROUP, me, everything)

    @pl.when(low & first_half)
    def _():
        with jax.named_scope("ready2"):
            pl.semaphore_wait(row_ready.at[2], GROUP // 2)
        send_to(near_high - GROUP // 2, near_high, everything)

    half_end = jnp.where(low, (middle + 1) * GROUP, rows)
    last = jnp.minimum((mine + 1) * GROUP, half_end)
    greeted = jnp.where(low, jnp.minimum((mine + 2) * GROUP, half_end), last)
    count = half_end - me - 1 - (greeted - last) + cols - 1 - my_col

    @pl.when(count > 0)
    def _():
        with jax.named_scope("ready0"):
            pl.semaphore_wait(row_ready.at[0], count)

    send_to(me + 1, last, everything)
    send_to(greeted, half_end, everything)

    @pl.when(low)
    def _():
        far = jnp.maximum(mine + 2, middle + 1) * GROUP
        with jax.named_scope("ready1"):
            pl.semaphore_wait(row_ready.at[1], rows - far)
        send_to(far, rows, everything)

    for copy in fetches:
        copy.wait()
    tall_x[...] = jnp.broadcast_to(sx[...], (LANES, nx)).T
    tall_y[...] = jnp.broadcast_to(sy[...], (LANES, ny)).T
    part_y = tall_y[pl.ds(my_col * half_y, half_y), :1]
    for x in range(share_x):
        part_x = tall_x[pl.ds(me * share_x + x, 1), :1]
        at = x % width * padded(nz)
        scale[x // width, :, at : at + nz] = 1.0 / (part_x + part_y + sz[...])

    for piece in everything:
        with jax.named_scope(f"rowwait{piece}"):
            row_all(piece).wait_recv()
        high, low = split(recv[piece].reshape(ny, LANES))
        stacked = jnp.concatenate([high, low], axis=0)
        parts = []
        for k in range(1, cols + 1):
            at = pl.multiple_of((my_col + k) % cols * half_y, half_y)
            table = jnp.concatenate([hy[pl.ds(at, half_y), :], hy[pl.ds(ny + at, half_y), :]], axis=0)
            both = jnp.dot(table, stacked, preferred_element_type=F32)
            parts.append(both[:half_y] + both[half_y:])
        for k in range(1, cols):
            mixed[piece, (my_col + k) % cols] = parts[k - 1]
        for k in range(1, cols):
            col_copy(piece, (my_col + k) % cols).start()
        if piece < pieces - 1:
            gathered[piece, my_col] = parts[-1]
        else:
            lines[my_col] = parts[-1]

    for piece in everything:
        with jax.named_scope(f"colwait{piece}"):
            col_all(piece).wait_recv()
        if piece < pieces - 1:
            last_axis(gathered.at[piece], scale[piece % quads], wz, early.at[piece])
        if piece == pieces - 2:
            sent = send.at[:, pl.ds(0, rows - 1)]
            pltpu.make_async_copy(sent, sent, row_send).wait()
    sent = mixed.at[:, pl.ds(0, cols - 1)]
    pltpu.make_async_copy(sent, sent, col_send).wait()


def last_axis(lines, scale, wz, out):
    cols, half_y, _ = lines.shape
    width, _, nz = out.shape
    line = jnp.concatenate([lines[c] for c in range(cols)], axis=1)
    high, low = split(line)
    both = jnp.dot(jnp.concatenate([high, low], axis=0), wz[0], preferred_element_type=F32)
    done = both[:half_y] + both[half_y:]
    done = done + jnp.dot(high, wz[1], preferred_element_type=F32)
    done = done * scale
    for j in range(width):
        out[j] = done[:, j * padded(nz) : j * padded(nz) + nz]


def last_kernel(lines, scale, early, wz, out, held, out_sem):
    pieces = early.shape[0] + 1
    quads, width = scale.shape[0], held.shape[0]
    copies = []
    for piece in range(pieces):
        if piece == pieces - 1:
            last_axis(lines, scale[piece % quads], wz, held)
        source = early.at[piece] if piece < pieces - 1 else held
        place = out.at[piece // quads, pl.ds(piece % quads * width, width)]
        copy = pltpu.make_async_copy(source, place, out_sem.at[piece])
        copy.start()
        copies.append(copy)
    with jax.named_scope("outwait"):
        for copy in copies:
            copy.wait()


def on_device(rows, cols, species, symbol_x, symbol_y, symbol_z):
    fields, nx, share_y, share_z = species.shape
    ny, nz = symbol_y.shape[0], symbol_z.shape[0]
    share_x, half_y = nx // rows, ny // cols
    width = LANES // share_z
    quads = share_x // width
    pieces = fields * quads
    hx, hy, wz = (jnp.asarray(t) for t in tables(rows, nx, ny, nz, share_z))
    dma = pltpu.SemaphoreType.DMA
    regular = pltpu.SemaphoreType.REGULAR
    width_z = width * padded(nz)
    vmem = pl.BlockSpec(memory_space=pltpu.VMEM)
    lines, scale, early = pl.pallas_call(
        functools.partial(kernel, rows, cols, ("row", "col")),
        out_shape=(
            jax.ShapeDtypeStruct((cols, half_y, LANES), F32),
            jax.ShapeDtypeStruct((quads, half_y, width_z), F32),
            jax.ShapeDtypeStruct((pieces - 1, width, half_y, nz), F32),
        ),
        in_specs=[pl.BlockSpec(memory_space=pl.ANY)] * 7,
        out_specs=(vmem, vmem, vmem),
        scratch_shapes=[
            pltpu.VMEM((fields, nx // LANES, share_z, share_y, LANES), F32),
            pltpu.VMEM((fields, share_y * share_z, 2 * nx), F32),
            pltpu.VMEM(hx.shape, BF16),
            pltpu.VMEM(hy.shape, BF16),
            pltpu.VMEM(wz.shape, BF16),
            pltpu.VMEM((1, nx), F32),
            pltpu.VMEM((1, ny), F32),
            pltpu.VMEM((1, nz), F32),
            pltpu.VMEM((pieces, rows, share_y, LANES), F32),
            pltpu.VMEM((pieces, rows, share_y, LANES), F32),
            pltpu.VMEM((pieces, cols, half_y, LANES), F32),
            pltpu.VMEM((pieces - 1, cols, half_y, LANES), F32),
            pltpu.VMEM((nx, LANES), F32),
            pltpu.VMEM((ny, LANES), F32),
            dma,
            dma((pieces,)),
            dma,
            dma((pieces,)),
            regular((3,)),
        ],
        compiler_params=pltpu.CompilerParams(collective_id=0, has_side_effects=True, vmem_limit_bytes=24 * 2**20),
    )(
        *(pltpu.with_memory_space_constraint(v, pltpu.HBM) for v in (jnp.transpose(species, (0, 2, 3, 1)), hx, hy,
        wz, symbol_x[None, :], symbol_y[None, :], symbol_z[None, :])),
    )
    return pl.pallas_call(
        last_kernel,
        out_shape=jax.ShapeDtypeStruct((fields, share_x, half_y, nz), F32),
        in_specs=[vmem, vmem, vmem, vmem],
        out_specs=pl.BlockSpec(memory_space=pl.ANY),
        scratch_shapes=[pltpu.VMEM((width, half_y, nz), F32), dma((pieces,))],
        compiler_params=pltpu.CompilerParams(vmem_limit_bytes=24 * 2**20),
    )(lines, scale, early, wz)


def solution(mesh):
    rows, cols = mesh.shape["row"], mesh.shape["col"]
    in_specs = (P(None, None, "row", "col"), P(), P(), P())
    out_specs = P(None, "row", "col", None)
    return jax.shard_map(
        functools.partial(on_device, rows, cols),
        mesh=mesh, in_specs=in_specs, out_specs=out_specs, check_vma=False,
    )
```

```python
import functools

import jax
import jax.numpy as jnp
import ml_dtypes
import numpy as np
from jax import lax
from jax.experimental import pallas as pl
from jax.experimental.pallas import tpu as pltpu
from jax.sharding import PartitionSpec as P

LANES = 128
GROUP = 4
F32, BF16 = jnp.float32, jnp.bfloat16
MESH = pl.DeviceIdType.MESH


def basis_table(count):
    odd = 2 * np.arange(count) + 1
    angle = np.pi / (4 * count) * (odd[:, None] * odd[None, :] % (8 * count))
    return np.cos(angle) * (2.0 / count) ** 0.5


def halves(table):
    high = table.astype(ml_dtypes.bfloat16)
    low = (table - high.astype(np.float64)).astype(ml_dtypes.bfloat16)
    return high, low


def split(values):
    high = values.astype(BF16)
    low = (values - high.astype(F32)).astype(BF16)
    return high, low


def padded(count):
    return -(-count // LANES) * LANES


def tables(rows, nx, ny, nz, share_z):
    width, half = LANES // share_z, share_z // 2
    share_x = nx // rows
    lane = np.arange(LANES)
    blocks = []
    for quad in range(share_x // width):
        for first in range(0, rows, half):
            column = lane[: LANES // 2]
            x = (first + column % half) * share_x + quad * width + column // half
            high, low = halves(basis_table(nx)[:, x])
            blocks += [high, low]
    table_x = np.tile(np.concatenate(blocks, axis=1), (2, 1))
    high, low = halves(basis_table(ny))
    table_y = np.block([[high, high], [low, low]])
    wide = np.zeros((nz // share_z, LANES, width, padded(nz)))
    for start in range(nz // share_z):
        z = start * share_z + lane % half + half * (lane // (LANES // 2))
        wide[start, lane, lane % (LANES // 2) // half, :nz] = basis_table(nz)[z]
    table_z = np.stack(halves(wide.reshape(-1, width * padded(nz))))
    return table_x, table_y, table_z


def kernel(
    rows, cols, names,
    species, hx_hbm, hy_hbm, wz_hbm, sx_hbm, sy_hbm, sz_hbm,
    lines, scale, early,
    xin, mid, hx, hy, wz, sx, sy, sz, send, recv, mixed, gathered, tall_x, tall_y,
    row_send, row_recv, col_send, col_recv, row_ready,
):
    row_name, col_name = names
    fields, _, _, nx = species.shape
    ny, nz = sy.shape[1], sz.shape[1]
    share_y, share_z = ny // rows, nz // cols
    share_x, half_y = nx // rows, ny // cols
    width, half = LANES // share_z, share_z // 2
    quads = share_x // width
    pieces = fields * quads
    groups = rows // GROUP
    middle = groups // 2 - 1
    me, my_col = lax.axis_index(row_name), lax.axis_index(col_name)
    mine = me // GROUP

    def fetch(source, target, semaphore, parts):
        step = source.shape[0] // parts
        for i in range(parts):
            span = pl.ds(i * step, step)
            pltpu.make_async_copy(source.at[span], target.at[span], semaphore).start()

    blocks = nx // LANES
    landed = (row_send, *([col_send] * (fields - 1)))

    def fetch_field(f):
        for b in range(blocks):
            for y in range(share_y):
                pltpu.make_async_copy(
                    species.at[f, y, :, pl.ds(b * LANES, LANES)], xin.at[f, b, :, y, :], landed[f]
                ).start()

    fetch(hx_hbm, hx, row_send, 4)
    fetch_field(0)

    barrier = pltpu.get_barrier_semaphore()

    def greet_row(t, carry):
        pl.semaphore_signal(barrier, inc=1, device_id={row_name: t}, device_id_type=MESH)
        return carry

    def greet_col(t, carry):
        pl.semaphore_signal(barrier, inc=1, device_id={col_name: t}, device_id_type=MESH)
        return carry

    low = mine <= middle
    back = (mine - 1) * GROUP
    past = (mine > 0) & (mine <= middle + 1)
    first_half = me % GROUP < GROUP // 2
    back_from = back + jnp.where(first_half, 0, GROUP // 2)
    lax.fori_loop(jnp.where(past, back_from, 0), jnp.where(past, back + GROUP, 0), greet_row, 0)
    lax.fori_loop(me + 1, rows, greet_row, 0)
    lax.fori_loop(my_col + 1, cols, greet_col, 0)
    for f in range(1, fields):
        fetch_field(f)
    rest = ((hy_hbm, hy), (wz_hbm, wz), (sx_hbm, sx), (sy_hbm, sy), (sz_hbm, sz))
    fetches = [pltpu.make_async_copy(a, b, col_send) for a, b in rest]

    def ready_row(t, carry):
        other = (~low & (t < (middle + 1) * GROUP)).astype(jnp.int32)
        other = jnp.where(past & (t >= back), jnp.where(t < back + GROUP, 2, other), other)
        pl.semaphore_signal(row_ready.at[other], inc=1, device_id={row_name: t}, device_id_type=MESH)
        return carry

    def ready_col(t, carry):
        pl.semaphore_signal(row_ready.at[0], inc=1, device_id={col_name: t}, device_id_type=MESH)
        return carry

    def meet():
        count = me + my_col + jnp.where(low, jnp.where(first_half, GROUP // 2, GROUP), 0)

        @pl.when(count > 0)
        def _():
            with jax.named_scope("barrier"):
                pl.semaphore_wait(barrier, count)

        lax.fori_loop(0, jnp.where(past, back_from, me), ready_row, 0)
        lax.fori_loop(jnp.where(past, mine * GROUP, me), me, ready_row, 0)
        lax.fori_loop(0, my_col, ready_col, 0)

    soon = (me % GROUP >= GROUP // 2) & ~low
    pl.when(soon)(meet)

    lane = lax.broadcasted_iota(jnp.int32, (share_y, LANES), 1)

    def row_copy(piece, target):
        return pltpu.make_async_remote_copy(
            src_ref=send.at[piece, target],
            dst_ref=recv.at[piece, me],
            send_sem=row_send,
            recv_sem=row_recv.at[piece],
            device_id={row_name: target},
            device_id_type=MESH,
        )

    def row_all(piece):
        return pltpu.make_async_remote_copy(
            src_ref=send.at[piece, pl.ds(0, rows - 1)],
            dst_ref=recv.at[piece, pl.ds(0, rows - 1)],
            send_sem=row_send,
            recv_sem=row_recv.at[piece],
            device_id={row_name: me},
            device_id_type=MESH,
        )

    def col_copy(piece, target):
        return pltpu.make_async_remote_copy(
            src_ref=mixed.at[piece, target],
            dst_ref=(gathered.at[piece, my_col] if piece < pieces - 1 else lines.at[my_col]),
            send_sem=col_send,
            recv_sem=col_recv.at[piece],
            device_id={col_name: target},
            device_id_type=MESH,
        )

    def col_all(piece):
        part = pl.ds(0, cols - 1)
        return pltpu.make_async_remote_copy(
            src_ref=mixed.at[piece, part],
            dst_ref=(gathered.at[piece, part] if piece < pieces - 1 else lines.at[part]),
            send_sem=col_send,
            recv_sem=col_recv.at[piece],
            device_id={col_name: my_col},
            device_id_type=MESH,
        )

    def send_to(least, most, some):
        for piece in some:

            def step(t, carry, piece=piece):
                row_copy(piece, t).start()
                return carry

            lax.fori_loop(least, most, step, 0)

    everything = range(pieces)
    front = jnp.minimum(mine, 1) * (GROUP // 2)
    near_high = (mine + 2) * GROUP
    def product(f):
        cut = [
            split(xin[f, b].reshape(share_z * share_y, LANES)) for b in range(blocks)
        ]
        line = jnp.concatenate([part for pair in zip(*cut) for part in pair], axis=1)
        size = half * share_y
        for at in (0, size):
            mid[f, at : at + size] = jnp.dot(
                line[at : at + size], hx[...], preferred_element_type=F32
            )

    def load(f):
        pltpu.make_async_copy(xin.at[f], xin.at[f], landed[f]).wait()

    with jax.named_scope("load"):
        pltpu.make_async_copy(hx_hbm, hx, row_send).wait()
        load(0)
    product(0)
    for piece in everything:
        f, quad = piece // quads, piece % quads
        if quad == quads - 1 and f + 1 < fields:
            load(f + 1)
            product(f + 1)
            if f + 2 == fields:
                for copy in fetches:
                    copy.start()
        for block in range(rows // half):
            at = (quad * (rows // half) + block) * LANES
            tiles = [
                mid[f, z * share_y : (z + 1) * share_y, at : at + LANES] for z in range(share_z)
            ]
            keep = lane < LANES // 2
            tiles = [
                jnp.where(keep, a, b) + pltpu.roll(jnp.where(keep, b, a), LANES // 2, 1)
                for a, b in zip(tiles[:half], tiles[half:])
            ]
            unit = 1
            while unit < half:
                radix = min(4, half // unit)
                place = lane // unit % radix
                turned = list(tiles)
                for i in range(half):
                    own = i // unit % radix
                    for other in range(radix):
                        source = tiles[i + (other - own) * unit]
                        if other != own:
                            source = pltpu.roll(source, (other - own) * unit % LANES, 1)
                        turned[i] = source if other == 0 else jnp.where(place == other, source, turned[i])
                tiles = turned
                unit *= radix
            for i in range(half):
                send[piece, block * half + i] = tiles[i]
        if piece == 0:
            pl.when(~soon & ~low)(meet)
        with jax.named_scope(f"near{piece}"):

            @pl.when(~low)
            def _():
                send_to(0, front, [piece])

            if piece >= quads - 1:
                some = range(quads) if piece == quads - 1 else [piece]

                @pl.when(low)
                def _():
                    if piece == quads - 1:
                        meet()
                    for one in some:
                        send_to(0, front, [one])
                        send_to(near_high - GROUP, near_high - jnp.where(first_half, GROUP // 2, 0), [one])

            recv[piece, me] = send[piece, me]

    across = (jnp.where(mine > 0, GROUP, 0), jnp.minimum(mine, middle + 1) * GROUP)

    def send_near(some):
        for g in reversed(range(middle + 1, groups)):

            @pl.when(g < mine)
            def _():
                send_to(g * GROUP, (g + 1) * GROUP, some)

    across_mid = (across[0] + across[1]) // 2
    for f in range(fields):
        some = range(f * quads, (f + 1) * quads)
        send_to(front, 2 * front, some)
        if f > 0:
            send_near(some[: quads // 2])
            send_to(across[0], across_mid, some)
            send_near(some[quads // 2 :])
            send_to(across_mid, across[1], some)
        else:
            send_near(some)
            send_to(*across, some)
    send_to(mine * GROUP, me, everything)

    @pl.when(low & first_half)
    def _():
        with jax.named_scope("ready2"):
            pl.semaphore_wait(row_ready.at[2], GROUP // 2)
        send_to(near_high - GROUP // 2, near_high, everything)

    half_end = jnp.where(low, (middle + 1) * GROUP, rows)
    last = jnp.minimum((mine + 1) * GROUP, half_end)
    greeted = jnp.where(low, jnp.minimum((mine + 2) * GROUP, half_end), last)
    count = half_end - me - 1 - (greeted - last) + cols - 1 - my_col

    @pl.when(count > 0)
    def _():
        with jax.named_scope("ready0"):
            pl.semaphore_wait(row_ready.at[0], count)

    send_to(me + 1, last, everything)
    send_to(greeted, half_end, everything)

    @pl.when(low)
    def _():
        far = jnp.maximum(mine + 2, middle + 1) * GROUP
        with jax.named_scope("ready1"):
            pl.semaphore_wait(row_ready.at[1], rows - far)
        send_to(far, rows, everything)

    for copy in fetches:
        copy.wait()
    tall_x[...] = jnp.broadcast_to(sx[...], (LANES, nx)).T
    tall_y[...] = jnp.broadcast_to(sy[...], (LANES, ny)).T
    part_y = tall_y[pl.ds(my_col * half_y, half_y), :1]
    for x in range(share_x):
        part_x = tall_x[pl.ds(me * share_x + x, 1), :1]
        at = x % width * padded(nz)
        scale[x // width, :, at : at + nz] = 1.0 / (part_x + part_y + sz[...])

    for piece in everything:
        with jax.named_scope(f"rowwait{piece}"):
            row_all(piece).wait_recv()
        high, low = split(recv[piece].reshape(ny, LANES))
        stacked = jnp.concatenate([high, low], axis=0)
        parts = []
        for k in range(1, cols + 1):
            at = pl.multiple_of((my_col + k) % cols * half_y, half_y)
            table = jnp.concatenate([hy[pl.ds(at, half_y), :], hy[pl.ds(ny + at, half_y), :]], axis=0)
            both = jnp.dot(table, stacked, preferred_element_type=F32)
            parts.append(both[:half_y] + both[half_y:])
        for k in range(1, cols):
            mixed[piece, (my_col + k) % cols] = parts[k - 1]
        for k in range(1, cols):
            col_copy(piece, (my_col + k) % cols).start()
        if piece < pieces - 1:
            gathered[piece, my_col] = parts[-1]
        else:
            lines[my_col] = parts[-1]

    for piece in everything:
        with jax.named_scope(f"colwait{piece}"):
            col_all(piece).wait_recv()
        if piece < pieces - 1:
            last_axis(gathered.at[piece], scale[piece % quads], wz, early.at[piece])
        if piece == pieces - 2:
            sent = send.at[:, pl.ds(0, rows - 1)]
            pltpu.make_async_copy(sent, sent, row_send).wait()
    sent = mixed.at[:, pl.ds(0, cols - 1)]
    pltpu.make_async_copy(sent, sent, col_send).wait()


def last_axis(lines, scale, wz, out):
    cols, half_y, _ = lines.shape
    width, _, nz = out.shape
    line = jnp.concatenate([lines[c] for c in range(cols)], axis=1)
    high, low = split(line)
    both = jnp.dot(jnp.concatenate([high, low], axis=0), wz[0], preferred_element_type=F32)
    done = both[:half_y] + both[half_y:]
    done = done + jnp.dot(high, wz[1], preferred_element_type=F32)
    done = done * scale
    for j in range(width):
        out[j] = done[:, j * padded(nz) : j * padded(nz) + nz]


def last_kernel(lines, scale, early, wz, out, held, out_sem):
    pieces = early.shape[0] + 1
    quads, width = scale.shape[0], held.shape[0]
    copies = []
    for piece in range(pieces):
        if piece == pieces - 1:
            last_axis(lines, scale[piece % quads], wz, held)
        source = early.at[piece] if piece < pieces - 1 else held
        place = out.at[piece // quads, pl.ds(piece % quads * width, width)]
        copy = pltpu.make_async_copy(source, place, out_sem.at[piece])
        copy.start()
        copies.append(copy)
    with jax.named_scope("outwait"):
        for copy in copies:
            copy.wait()


def on_device(rows, cols, species, symbol_x, symbol_y, symbol_z):
    fields, nx, share_y, share_z = species.shape
    ny, nz = symbol_y.shape[0], symbol_z.shape[0]
    share_x, half_y = nx // rows, ny // cols
    width = LANES // share_z
    quads = share_x // width
    pieces = fields * quads
    hx, hy, wz = (jnp.asarray(t) for t in tables(rows, nx, ny, nz, share_z))
    dma = pltpu.SemaphoreType.DMA
    regular = pltpu.SemaphoreType.REGULAR
    width_z = width * padded(nz)
    vmem = pl.BlockSpec(memory_space=pltpu.VMEM)
    lines, scale, early = pl.pallas_call(
        functools.partial(kernel, rows, cols, ("row", "col")),
        out_shape=(
            jax.ShapeDtypeStruct((cols, half_y, LANES), F32),
            jax.ShapeDtypeStruct((quads, half_y, width_z), F32),
            jax.ShapeDtypeStruct((pieces - 1, width, half_y, nz), F32),
        ),
        in_specs=[pl.BlockSpec(memory_space=pl.ANY)] * 7,
        out_specs=(vmem, vmem, vmem),
        scratch_shapes=[
            pltpu.VMEM((fields, nx // LANES, share_z, share_y, LANES), F32),
            pltpu.VMEM((fields, share_y * share_z, 2 * nx), F32),
            pltpu.VMEM(hx.shape, BF16),
            pltpu.VMEM(hy.shape, BF16),
            pltpu.VMEM(wz.shape, BF16),
            pltpu.VMEM((1, nx), F32),
            pltpu.VMEM((1, ny), F32),
            pltpu.VMEM((1, nz), F32),
            pltpu.VMEM((pieces, rows, share_y, LANES), F32),
            pltpu.VMEM((pieces, rows, share_y, LANES), F32),
            pltpu.VMEM((pieces, cols, half_y, LANES), F32),
            pltpu.VMEM((pieces - 1, cols, half_y, LANES), F32),
            pltpu.VMEM((nx, LANES), F32),
            pltpu.VMEM((ny, LANES), F32),
            dma,
            dma((pieces,)),
            dma,
            dma((pieces,)),
            regular((3,)),
        ],
        compiler_params=pltpu.CompilerParams(collective_id=0, has_side_effects=True, vmem_limit_bytes=24 * 2**20),
    )(
        *(pltpu.with_memory_space_constraint(v, pltpu.HBM) for v in (jnp.transpose(species, (0, 2, 3, 1)), hx, hy,
        wz, symbol_x[None, :], symbol_y[None, :], symbol_z[None, :])),
    )
    return pl.pallas_call(
        last_kernel,
        out_shape=jax.ShapeDtypeStruct((fields, share_x, half_y, nz), F32),
        in_specs=[vmem, vmem, vmem, vmem],
        out_specs=pl.BlockSpec(memory_space=pl.ANY),
        scratch_shapes=[pltpu.VMEM((width, half_y, nz), F32), dma((pieces,))],
        compiler_params=pltpu.CompilerParams(vmem_limit_bytes=24 * 2**20),
    )(lines, scale, early, wz)


def solution(mesh):
    rows, cols = mesh.shape["row"], mesh.shape["col"]
    in_specs = (P(None, None, "row", "col"), P(), P(), P())
    out_specs = P(None, "row", "col", None)
    return jax.shard_map(
        functools.partial(on_device, rows, cols),
        mesh=mesh, in_specs=in_specs, out_specs=out_specs, check_vma=False,
    )
```

```python
import functools

import jax
import jax.numpy as jnp
import ml_dtypes
import numpy as np
from jax import lax
from jax.experimental import pallas as pl
from jax.experimental.pallas import tpu as pltpu
from jax.sharding import PartitionSpec as P

LANES = 128
GROUP = 4
F32, BF16 = jnp.float32, jnp.bfloat16
MESH = pl.DeviceIdType.MESH


def basis_table(count):
    odd = 2 * np.arange(count) + 1
    angle = np.pi / (4 * count) * (odd[:, None] * odd[None, :] % (8 * count))
    return np.cos(angle) * (2.0 / count) ** 0.5


def halves(table):
    high = table.astype(ml_dtypes.bfloat16)
    low = (table - high.astype(np.float64)).astype(ml_dtypes.bfloat16)
    return high, low


def split(values):
    high = values.astype(BF16)
    low = (values - high.astype(F32)).astype(BF16)
    return high, low


def padded(count):
    return -(-count // LANES) * LANES


def tables(rows, nx, ny, nz, share_z):
    width, half = LANES // share_z, share_z // 2
    share_x = nx // rows
    lane = np.arange(LANES)
    blocks = []
    for quad in range(share_x // width):
        for first in range(0, rows, half):
            column = lane[: LANES // 2]
            x = (first + column % half) * share_x + quad * width + column // half
            high, low = halves(basis_table(nx)[:, x])
            blocks += [high, low]
    table_x = np.tile(np.concatenate(blocks, axis=1), (2, 1))
    high, low = halves(basis_table(ny))
    table_y = np.block([[high, high], [low, low]])
    wide = np.zeros((nz // share_z, LANES, width, padded(nz)))
    for start in range(nz // share_z):
        z = start * share_z + lane % half + half * (lane // (LANES // 2))
        wide[start, lane, lane % (LANES // 2) // half, :nz] = basis_table(nz)[z]
    table_z = np.stack(halves(wide.reshape(-1, width * padded(nz))))
    return table_x, table_y, table_z


def kernel(
    rows, cols, names,
    species, hx_hbm, hy_hbm, wz_hbm, sx_hbm, sy_hbm, sz_hbm,
    lines, scale, early,
    xin, mid, hx, hy, wz, sx, sy, sz, send, recv, mixed, gathered, tall_x, tall_y,
    row_send, row_recv, col_send, col_recv, row_ready,
):
    row_name, col_name = names
    fields, _, _, nx = species.shape
    ny, nz = sy.shape[1], sz.shape[1]
    share_y, share_z = ny // rows, nz // cols
    share_x, half_y = nx // rows, ny // cols
    width, half = LANES // share_z, share_z // 2
    quads = share_x // width
    pieces = fields * quads
    groups = rows // GROUP
    middle = groups // 2 - 1
    me, my_col = lax.axis_index(row_name), lax.axis_index(col_name)
    mine = me // GROUP

    def fetch(source, target, semaphore, parts):
        step = source.shape[0] // parts
        for i in range(parts):
            span = pl.ds(i * step, step)
            pltpu.make_async_copy(source.at[span], target.at[span], semaphore).start()

    blocks = nx // LANES
    landed = (row_send, *([col_send] * (fields - 1)))

    def fetch_field(f):
        for b in range(blocks):
            for y in range(share_y):
                pltpu.make_async_copy(
                    species.at[f, y, :, pl.ds(b * LANES, LANES)], xin.at[f, b, :, y, :], landed[f]
                ).start()

    fetch(hx_hbm, hx, row_send, 4)
    fetch_field(0)

    barrier = pltpu.get_barrier_semaphore()

    def greet_row(t, carry):
        pl.semaphore_signal(barrier, inc=1, device_id={row_name: t}, device_id_type=MESH)
        return carry

    def greet_col(t, carry):
        pl.semaphore_signal(barrier, inc=1, device_id={col_name: t}, device_id_type=MESH)
        return carry

    low = mine <= middle
    back = (mine - 1) * GROUP
    past = (mine > 0) & (mine <= middle + 1)
    first_half = me % GROUP < GROUP // 2
    back_from = back + jnp.where(first_half, 0, GROUP // 2)
    lax.fori_loop(jnp.where(past, back_from, 0), jnp.where(past, back + GROUP, 0), greet_row, 0)
    lax.fori_loop(me + 1, rows, greet_row, 0)
    lax.fori_loop(my_col + 1, cols, greet_col, 0)
    for f in range(1, fields):
        fetch_field(f)
    rest = ((hy_hbm, hy), (wz_hbm, wz), (sx_hbm, sx), (sy_hbm, sy), (sz_hbm, sz))
    fetches = [pltpu.make_async_copy(a, b, col_send) for a, b in rest]

    def ready_row(t, carry):
        other = (~low & (t < (middle + 1) * GROUP)).astype(jnp.int32)
        other = jnp.where(past & (t >= back), jnp.where(t < back + GROUP, 2, other), other)
        pl.semaphore_signal(row_ready.at[other], inc=1, device_id={row_name: t}, device_id_type=MESH)
        return carry

    def ready_col(t, carry):
        pl.semaphore_signal(row_ready.at[0], inc=1, device_id={col_name: t}, device_id_type=MESH)
        return carry

    def meet():
        count = me + my_col + jnp.where(low, jnp.where(first_half, GROUP // 2, GROUP), 0)

        @pl.when(count > 0)
        def _():
            with jax.named_scope("barrier"):
                pl.semaphore_wait(barrier, count)

        lax.fori_loop(0, jnp.where(past, back_from, me), ready_row, 0)
        lax.fori_loop(jnp.where(past, mine * GROUP, me), me, ready_row, 0)
        lax.fori_loop(0, my_col, ready_col, 0)

    soon = (me % GROUP >= GROUP // 2) & ~low
    pl.when(soon)(meet)

    lane = lax.broadcasted_iota(jnp.int32, (share_y, LANES), 1)

    def row_copy(piece, target):
        return pltpu.make_async_remote_copy(
            src_ref=send.at[piece, target],
            dst_ref=recv.at[piece, me],
            send_sem=row_send,
            recv_sem=row_recv.at[piece],
            device_id={row_name: target},
            device_id_type=MESH,
        )

    def row_all(piece):
        return pltpu.make_async_remote_copy(
            src_ref=send.at[piece, pl.ds(0, rows - 1)],
            dst_ref=recv.at[piece, pl.ds(0, rows - 1)],
            send_sem=row_send,
            recv_sem=row_recv.at[piece],
            device_id={row_name: me},
            device_id_type=MESH,
        )

    def col_copy(piece, target):
        return pltpu.make_async_remote_copy(
            src_ref=mixed.at[piece, target],
            dst_ref=(gathered.at[piece, my_col] if piece < pieces - 1 else lines.at[my_col]),
            send_sem=col_send,
            recv_sem=col_recv.at[piece],
            device_id={col_name: target},
            device_id_type=MESH,
        )

    def col_all(piece):
        part = pl.ds(0, cols - 1)
        return pltpu.make_async_remote_copy(
            src_ref=mixed.at[piece, part],
            dst_ref=(gathered.at[piece, part] if piece < pieces - 1 else lines.at[part]),
            send_sem=col_send,
            recv_sem=col_recv.at[piece],
            device_id={col_name: my_col},
            device_id_type=MESH,
        )

    def send_to(least, most, some):
        for piece in some:

            def step(t, carry, piece=piece):
                row_copy(piece, t).start()
                return carry

            lax.fori_loop(least, most, step, 0)

    everything = range(pieces)
    front = jnp.minimum(mine, 1) * (GROUP // 2)
    near_high = (mine + 2) * GROUP
    def product(f):
        cut = [
            split(xin[f, b].reshape(share_z * share_y, LANES)) for b in range(blocks)
        ]
        line = jnp.concatenate([part for pair in zip(*cut) for part in pair], axis=1)
        size = half * share_y
        for at in (0, size):
            mid[f, at : at + size] = jnp.dot(
                line[at : at + size], hx[...], preferred_element_type=F32
            )

    def load(f):
        pltpu.make_async_copy(xin.at[f], xin.at[f], landed[f]).wait()

    with jax.named_scope("load"):
        pltpu.make_async_copy(hx_hbm, hx, row_send).wait()
        load(0)
    product(0)
    for piece in everything:
        f, quad = piece // quads, piece % quads
        if quad == quads - 1 and f + 1 < fields:
            load(f + 1)
            product(f + 1)
            if f + 2 == fields:
                for copy in fetches:
                    copy.start()
        for block in range(rows // half):
            at = (quad * (rows // half) + block) * LANES
            tiles = [
                mid[f, z * share_y : (z + 1) * share_y, at : at + LANES] for z in range(share_z)
            ]
            keep = lane < LANES // 2
            tiles = [
                jnp.where(keep, a, b) + pltpu.roll(jnp.where(keep, b, a), LANES // 2, 1)
                for a, b in zip(tiles[:half], tiles[half:])
            ]
            unit = 1
            while unit < half:
                radix = min(4, half // unit)
                place = lane // unit % radix
                turned = list(tiles)
                for i in range(half):
                    own = i // unit % radix
                    for other in range(radix):
                        source = tiles[i + (other - own) * unit]
                        if other != own:
                            source = pltpu.roll(source, (other - own) * unit % LANES, 1)
                        turned[i] = source if other == 0 else jnp.where(place == other, source, turned[i])
                tiles = turned
                unit *= radix
            for i in range(half):
                send[piece, block * half + i] = tiles[i]
        if piece == 0:
            pl.when(~soon & ~low)(meet)
        with jax.named_scope(f"near{piece}"):

            @pl.when(~low)
            def _():
                send_to(0, front, [piece])

            if piece >= quads - 1:
                some = range(quads) if piece == quads - 1 else [piece]

                @pl.when(low)
                def _():
                    if piece == quads - 1:
                        meet()
                    for one in some:
                        send_to(0, front, [one])
                        send_to(near_high - GROUP, near_high - jnp.where(first_half, GROUP // 2, 0), [one])


    across = (jnp.where(mine > 0, GROUP, 0), jnp.minimum(mine, middle + 1) * GROUP)

    def send_near(some):
        for g in reversed(range(middle + 1, groups)):

            @pl.when(g < mine)
            def _():
                send_to(g * GROUP, (g + 1) * GROUP, some)

    across_mid = (across[0] + across[1]) // 2
    for f in range(fields):
        some = range(f * quads, (f + 1) * quads)
        send_to(front, 2 * front, some)
        if f > 0:
            send_near(some[: quads // 2])
            send_to(across[0], across_mid, some)
            send_near(some[quads // 2 :])
            send_to(across_mid, across[1], some)
        else:
            send_near(some)
            send_to(*across, some)
    send_to(mine * GROUP, me, everything)
    for piece in everything:
        recv[piece, me] = send[piece, me]

    @pl.when(low & first_half)
    def _():
        with jax.named_scope("ready2"):
            pl.semaphore_wait(row_ready.at[2], GROUP // 2)
        send_to(near_high - GROUP // 2, near_high, everything)

    half_end = jnp.where(low, (middle + 1) * GROUP, rows)
    last = jnp.minimum((mine + 1) * GROUP, half_end)
    greeted = jnp.where(low, jnp.minimum((mine + 2) * GROUP, half_end), last)
    count = half_end - me - 1 - (greeted - last) + cols - 1 - my_col

    @pl.when(count > 0)
    def _():
        with jax.named_scope("ready0"):
            pl.semaphore_wait(row_ready.at[0], count)

    send_to(me + 1, last, everything)
    send_to(greeted, half_end, everything)

    @pl.when(low)
    def _():
        far = jnp.maximum(mine + 2, middle + 1) * GROUP
        with jax.named_scope("ready1"):
            pl.semaphore_wait(row_ready.at[1], rows - far)
        send_to(far, rows, everything)

    for copy in fetches:
        copy.wait()
    tall_x[...] = jnp.broadcast_to(sx[...], (LANES, nx)).T
    tall_y[...] = jnp.broadcast_to(sy[...], (LANES, ny)).T
    part_y = tall_y[pl.ds(my_col * half_y, half_y), :1]
    for x in range(share_x):
        part_x = tall_x[pl.ds(me * share_x + x, 1), :1]
        at = x % width * padded(nz)
        scale[x // width, :, at : at + nz] = 1.0 / (part_x + part_y + sz[...])

    for piece in everything:
        with jax.named_scope(f"rowwait{piece}"):
            row_all(piece).wait_recv()
        high, low = split(recv[piece].reshape(ny, LANES))
        stacked = jnp.concatenate([high, low], axis=0)
        parts = []
        for k in range(1, cols + 1):
            at = pl.multiple_of((my_col + k) % cols * half_y, half_y)
            table = jnp.concatenate([hy[pl.ds(at, half_y), :], hy[pl.ds(ny + at, half_y), :]], axis=0)
            both = jnp.dot(table, stacked, preferred_element_type=F32)
            parts.append(both[:half_y] + both[half_y:])
        for k in range(1, cols):
            mixed[piece, (my_col + k) % cols] = parts[k - 1]
        for k in range(1, cols):
            col_copy(piece, (my_col + k) % cols).start()
        if piece < pieces - 1:
            gathered[piece, my_col] = parts[-1]
        else:
            lines[my_col] = parts[-1]

    for piece in everything:
        with jax.named_scope(f"colwait{piece}"):
            col_all(piece).wait_recv()
        if piece < pieces - 1:
            last_axis(gathered.at[piece], scale[piece % quads], wz, early.at[piece])
        if piece == pieces - 2:
            sent = send.at[:, pl.ds(0, rows - 1)]
            pltpu.make_async_copy(sent, sent, row_send).wait()
    sent = mixed.at[:, pl.ds(0, cols - 1)]
    pltpu.make_async_copy(sent, sent, col_send).wait()


def last_axis(lines, scale, wz, out):
    cols, half_y, _ = lines.shape
    width, _, nz = out.shape
    line = jnp.concatenate([lines[c] for c in range(cols)], axis=1)
    high, low = split(line)
    both = jnp.dot(jnp.concatenate([high, low], axis=0), wz[0], preferred_element_type=F32)
    done = both[:half_y] + both[half_y:]
    done = done + jnp.dot(high, wz[1], preferred_element_type=F32)
    done = done * scale
    for j in range(width):
        out[j] = done[:, j * padded(nz) : j * padded(nz) + nz]


def last_kernel(lines, scale, early, wz, out, held, out_sem):
    pieces = early.shape[0] + 1
    quads, width = scale.shape[0], held.shape[0]
    copies = []
    for piece in range(pieces):
        if piece == pieces - 1:
            last_axis(lines, scale[piece % quads], wz, held)
        source = early.at[piece] if piece < pieces - 1 else held
        place = out.at[piece // quads, pl.ds(piece % quads * width, width)]
        copy = pltpu.make_async_copy(source, place, out_sem.at[piece])
        copy.start()
        copies.append(copy)
    with jax.named_scope("outwait"):
        for copy in copies:
            copy.wait()


def on_device(rows, cols, species, symbol_x, symbol_y, symbol_z):
    fields, nx, share_y, share_z = species.shape
    ny, nz = symbol_y.shape[0], symbol_z.shape[0]
    share_x, half_y = nx // rows, ny // cols
    width = LANES // share_z
    quads = share_x // width
    pieces = fields * quads
    hx, hy, wz = (jnp.asarray(t) for t in tables(rows, nx, ny, nz, share_z))
    dma = pltpu.SemaphoreType.DMA
    regular = pltpu.SemaphoreType.REGULAR
    width_z = width * padded(nz)
    vmem = pl.BlockSpec(memory_space=pltpu.VMEM)
    lines, scale, early = pl.pallas_call(
        functools.partial(kernel, rows, cols, ("row", "col")),
        out_shape=(
            jax.ShapeDtypeStruct((cols, half_y, LANES), F32),
            jax.ShapeDtypeStruct((quads, half_y, width_z), F32),
            jax.ShapeDtypeStruct((pieces - 1, width, half_y, nz), F32),
        ),
        in_specs=[pl.BlockSpec(memory_space=pl.ANY)] * 7,
        out_specs=(vmem, vmem, vmem),
        scratch_shapes=[
            pltpu.VMEM((fields, nx // LANES, share_z, share_y, LANES), F32),
            pltpu.VMEM((fields, share_y * share_z, 2 * nx), F32),
            pltpu.VMEM(hx.shape, BF16),
            pltpu.VMEM(hy.shape, BF16),
            pltpu.VMEM(wz.shape, BF16),
            pltpu.VMEM((1, nx), F32),
            pltpu.VMEM((1, ny), F32),
            pltpu.VMEM((1, nz), F32),
            pltpu.VMEM((pieces, rows, share_y, LANES), F32),
            pltpu.VMEM((pieces, rows, share_y, LANES), F32),
            pltpu.VMEM((pieces, cols, half_y, LANES), F32),
            pltpu.VMEM((pieces - 1, cols, half_y, LANES), F32),
            pltpu.VMEM((nx, LANES), F32),
            pltpu.VMEM((ny, LANES), F32),
            dma,
            dma((pieces,)),
            dma,
            dma((pieces,)),
            regular((3,)),
        ],
        compiler_params=pltpu.CompilerParams(collective_id=0, has_side_effects=True, vmem_limit_bytes=24 * 2**20),
    )(
        *(pltpu.with_memory_space_constraint(v, pltpu.HBM) for v in (jnp.transpose(species, (0, 2, 3, 1)), hx, hy,
        wz, symbol_x[None, :], symbol_y[None, :], symbol_z[None, :])),
    )
    return pl.pallas_call(
        last_kernel,
        out_shape=jax.ShapeDtypeStruct((fields, share_x, half_y, nz), F32),
        in_specs=[vmem, vmem, vmem, vmem],
        out_specs=pl.BlockSpec(memory_space=pl.ANY),
        scratch_shapes=[pltpu.VMEM((width, half_y, nz), F32), dma((pieces,))],
        compiler_params=pltpu.CompilerParams(vmem_limit_bytes=24 * 2**20),
    )(lines, scale, early, wz)


def solution(mesh):
    rows, cols = mesh.shape["row"], mesh.shape["col"]
    in_specs = (P(None, None, "row", "col"), P(), P(), P())
    out_specs = P(None, "row", "col", None)
    return jax.shard_map(
        functools.partial(on_device, rows, cols),
        mesh=mesh, in_specs=in_specs, out_specs=out_specs, check_vma=False,
    )
```

```python
import functools

import jax
import jax.numpy as jnp
import ml_dtypes
import numpy as np
from jax import lax
from jax.experimental import pallas as pl
from jax.experimental.pallas import tpu as pltpu
from jax.sharding import PartitionSpec as P

LANES = 128
GROUP = 4
F32, BF16 = jnp.float32, jnp.bfloat16
MESH = pl.DeviceIdType.MESH


def basis_table(count):
    odd = 2 * np.arange(count) + 1
    angle = np.pi / (4 * count) * (odd[:, None] * odd[None, :] % (8 * count))
    return np.cos(angle) * (2.0 / count) ** 0.5


def halves(table):
    high = table.astype(ml_dtypes.bfloat16)
    low = (table - high.astype(np.float64)).astype(ml_dtypes.bfloat16)
    return high, low


def split(values):
    high = values.astype(BF16)
    low = (values - high.astype(F32)).astype(BF16)
    return high, low


def padded(count):
    return -(-count // LANES) * LANES


def tables(rows, nx, ny, nz, share_z):
    width, half = LANES // share_z, share_z // 2
    share_x = nx // rows
    lane = np.arange(LANES)
    blocks = []
    for quad in range(share_x // width):
        for first in range(0, rows, half):
            column = lane[: LANES // 2]
            x = (first + column % half) * share_x + quad * width + column // half
            high, low = halves(basis_table(nx)[:, x])
            blocks += [high, low]
    table_x = np.tile(np.concatenate(blocks, axis=1), (2, 1))
    high, low = halves(basis_table(ny))
    table_y = np.block([[high, high], [low, low]])
    wide = np.zeros((nz // share_z, LANES, width, padded(nz)))
    for start in range(nz // share_z):
        z = start * share_z + lane % half + half * (lane // (LANES // 2))
        wide[start, lane, lane % (LANES // 2) // half, :nz] = basis_table(nz)[z]
    table_z = np.stack(halves(wide.reshape(-1, width * padded(nz))))
    return table_x, table_y, table_z


def kernel(
    rows, cols, names,
    species, hx_hbm, hy_hbm, wz_hbm, sx_hbm, sy_hbm, sz_hbm,
    lines, scale, early,
    xin, mid, hx, hy, wz, sx, sy, sz, send, recv, mixed, gathered, tall_x, tall_y,
    row_send, row_recv, col_send, col_recv, row_ready,
):
    row_name, col_name = names
    fields, _, _, nx = species.shape
    ny, nz = sy.shape[1], sz.shape[1]
    share_y, share_z = ny // rows, nz // cols
    share_x, half_y = nx // rows, ny // cols
    width, half = LANES // share_z, share_z // 2
    quads = share_x // width
    pieces = fields * quads
    groups = rows // GROUP
    middle = groups // 2 - 1
    me, my_col = lax.axis_index(row_name), lax.axis_index(col_name)
    mine = me // GROUP

    def fetch(source, target, semaphore, parts):
        step = source.shape[0] // parts
        for i in range(parts):
            span = pl.ds(i * step, step)
            pltpu.make_async_copy(source.at[span], target.at[span], semaphore).start()

    blocks = nx // LANES
    landed = (row_send, *([col_send] * (fields - 1)))

    def fetch_field(f):
        for b in range(blocks):
            for y in range(share_y):
                pltpu.make_async_copy(
                    species.at[f, y, :, pl.ds(b * LANES, LANES)], xin.at[f, b, :, y, :], landed[f]
                ).start()

    fetch(hx_hbm, hx, row_send, 4)
    fetch_field(0)

    barrier = pltpu.get_barrier_semaphore()

    def greet_row(t, carry):
        pl.semaphore_signal(barrier, inc=1, device_id={row_name: t}, device_id_type=MESH)
        return carry

    def greet_col(t, carry):
        pl.semaphore_signal(barrier, inc=1, device_id={col_name: t}, device_id_type=MESH)
        return carry

    low = mine <= middle
    back = (mine - 1) * GROUP
    past = (mine > 0) & (mine <= middle + 1)
    first_half = me % GROUP < GROUP // 2
    back_from = back + jnp.where(first_half, 0, GROUP // 2)
    lax.fori_loop(jnp.where(past, back_from, 0), jnp.where(past, back + GROUP, 0), greet_row, 0)
    lax.fori_loop(me + 1, rows, greet_row, 0)
    lax.fori_loop(my_col + 1, cols, greet_col, 0)
    for f in range(1, fields):
        fetch_field(f)
    rest = ((hy_hbm, hy), (wz_hbm, wz), (sx_hbm, sx), (sy_hbm, sy), (sz_hbm, sz))
    fetches = [pltpu.make_async_copy(a, b, col_send) for a, b in rest]

    def ready_row(t, carry):
        other = (~low & (t < (middle + 1) * GROUP)).astype(jnp.int32)
        other = jnp.where(past & (t >= back), jnp.where(t < back + GROUP, 2, other), other)
        pl.semaphore_signal(row_ready.at[other], inc=1, device_id={row_name: t}, device_id_type=MESH)
        return carry

    def ready_col(t, carry):
        pl.semaphore_signal(row_ready.at[0], inc=1, device_id={col_name: t}, device_id_type=MESH)
        return carry

    def meet():
        count = me + my_col + jnp.where(low, jnp.where(first_half, GROUP // 2, GROUP), 0)

        @pl.when(count > 0)
        def _():
            with jax.named_scope("barrier"):
                pl.semaphore_wait(barrier, count)

        lax.fori_loop(0, jnp.where(past, back_from, me), ready_row, 0)
        lax.fori_loop(jnp.where(past, mine * GROUP, me), me, ready_row, 0)
        lax.fori_loop(0, my_col, ready_col, 0)

    soon = (me % GROUP >= GROUP // 2) & ~low
    pl.when(soon)(meet)

    lane = lax.broadcasted_iota(jnp.int32, (share_y, LANES), 1)

    def row_copy(piece, target):
        return pltpu.make_async_remote_copy(
            src_ref=send.at[piece, target],
            dst_ref=recv.at[piece, me],
            send_sem=row_send,
            recv_sem=row_recv.at[piece],
            device_id={row_name: target},
            device_id_type=MESH,
        )

    def row_all(piece):
        return pltpu.make_async_remote_copy(
            src_ref=send.at[piece, pl.ds(0, rows - 1)],
            dst_ref=recv.at[piece, pl.ds(0, rows - 1)],
            send_sem=row_send,
            recv_sem=row_recv.at[piece],
            device_id={row_name: me},
            device_id_type=MESH,
        )

    def col_copy(piece, target):
        return pltpu.make_async_remote_copy(
            src_ref=mixed.at[piece, target],
            dst_ref=(gathered.at[piece, my_col] if piece < pieces - 1 else lines.at[my_col]),
            send_sem=col_send,
            recv_sem=col_recv.at[piece],
            device_id={col_name: target},
            device_id_type=MESH,
        )

    def col_all(piece):
        part = pl.ds(0, cols - 1)
        return pltpu.make_async_remote_copy(
            src_ref=mixed.at[piece, part],
            dst_ref=(gathered.at[piece, part] if piece < pieces - 1 else lines.at[part]),
            send_sem=col_send,
            recv_sem=col_recv.at[piece],
            device_id={col_name: my_col},
            device_id_type=MESH,
        )

    def send_to(least, most, some):
        for piece in some:
            for parity in (0, 1):

                def step(t, carry, piece=piece, parity=parity):
                    row_copy(piece, least + 2 * t + parity).start()
                    return carry

                lax.fori_loop(0, (most - least + 1 - parity) // 2, step, 0)

    everything = range(pieces)
    front = jnp.minimum(mine, 1) * (GROUP // 2)
    near_high = (mine + 2) * GROUP
    def product(f):
        cut = [
            split(xin[f, b].reshape(share_z * share_y, LANES)) for b in range(blocks)
        ]
        line = jnp.concatenate([part for pair in zip(*cut) for part in pair], axis=1)
        size = half * share_y
        for at in (0, size):
            mid[f, at : at + size] = jnp.dot(
                line[at : at + size], hx[...], preferred_element_type=F32
            )

    def load(f):
        pltpu.make_async_copy(xin.at[f], xin.at[f], landed[f]).wait()

    with jax.named_scope("load"):
        pltpu.make_async_copy(hx_hbm, hx, row_send).wait()
        load(0)
    product(0)
    for piece in everything:
        f, quad = piece // quads, piece % quads
        if quad == quads - 1 and f + 1 < fields:
            load(f + 1)
            product(f + 1)
            if f + 2 == fields:
                for copy in fetches:
                    copy.start()
        for block in range(rows // half):
            at = (quad * (rows // half) + block) * LANES
            tiles = [
                mid[f, z * share_y : (z + 1) * share_y, at : at + LANES] for z in range(share_z)
            ]
            keep = lane < LANES // 2
            tiles = [
                jnp.where(keep, a, b) + pltpu.roll(jnp.where(keep, b, a), LANES // 2, 1)
                for a, b in zip(tiles[:half], tiles[half:])
            ]
            unit = 1
            while unit < half:
                radix = min(4, half // unit)
                place = lane // unit % radix
                turned = list(tiles)
                for i in range(half):
                    own = i // unit % radix
                    for other in range(radix):
                        source = tiles[i + (other - own) * unit]
                        if other != own:
                            source = pltpu.roll(source, (other - own) * unit % LANES, 1)
                        turned[i] = source if other == 0 else jnp.where(place == other, source, turned[i])
                tiles = turned
                unit *= radix
            for i in range(half):
                send[piece, block * half + i] = tiles[i]
        if piece == 0:
            pl.when(~soon & ~low)(meet)
        with jax.named_scope(f"near{piece}"):

            @pl.when(~low)
            def _():
                send_to(0, front, [piece])

            if piece >= quads - 1:
                some = range(quads) if piece == quads - 1 else [piece]

                @pl.when(low)
                def _():
                    if piece == quads - 1:
                        meet()
                    for one in some:
                        send_to(0, front, [one])
                        send_to(near_high - GROUP, near_high - jnp.where(first_half, GROUP // 2, 0), [one])

            recv[piece, me] = send[piece, me]

    across = (jnp.where(mine > 0, GROUP, 0), jnp.minimum(mine, middle + 1) * GROUP)

    def send_near(some):
        for g in reversed(range(middle + 1, groups)):

            @pl.when(g < mine)
            def _():
                send_to(g * GROUP, (g + 1) * GROUP, some)

    across_mid = (across[0] + across[1]) // 2
    for f in range(fields):
        some = range(f * quads, (f + 1) * quads)
        send_to(front, 2 * front, some)
        if f > 0:
            send_near(some[: quads // 2])
            send_to(across[0], across_mid, some)
            send_near(some[quads // 2 :])
            send_to(across_mid, across[1], some)
        else:
            send_near(some)
            send_to(*across, some)
    send_to(mine * GROUP, me, everything)

    @pl.when(low & first_half)
    def _():
        with jax.named_scope("ready2"):
            pl.semaphore_wait(row_ready.at[2], GROUP // 2)
        send_to(near_high - GROUP // 2, near_high, everything)

    half_end = jnp.where(low, (middle + 1) * GROUP, rows)
    last = jnp.minimum((mine + 1) * GROUP, half_end)
    greeted = jnp.where(low, jnp.minimum((mine + 2) * GROUP, half_end), last)
    count = half_end - me - 1 - (greeted - last) + cols - 1 - my_col

    @pl.when(count > 0)
    def _():
        with jax.named_scope("ready0"):
            pl.semaphore_wait(row_ready.at[0], count)

    send_to(me + 1, last, everything)
    send_to(greeted, half_end, everything)

    @pl.when(low)
    def _():
        far = jnp.maximum(mine + 2, middle + 1) * GROUP
        with jax.named_scope("ready1"):
            pl.semaphore_wait(row_ready.at[1], rows - far)
        send_to(far, rows, everything)

    for copy in fetches:
        copy.wait()
    tall_x[...] = jnp.broadcast_to(sx[...], (LANES, nx)).T
    tall_y[...] = jnp.broadcast_to(sy[...], (LANES, ny)).T
    part_y = tall_y[pl.ds(my_col * half_y, half_y), :1]
    for x in range(share_x):
        part_x = tall_x[pl.ds(me * share_x + x, 1), :1]
        at = x % width * padded(nz)
        scale[x // width, :, at : at + nz] = 1.0 / (part_x + part_y + sz[...])

    for piece in everything:
        with jax.named_scope(f"rowwait{piece}"):
            row_all(piece).wait_recv()
        high, low = split(recv[piece].reshape(ny, LANES))
        stacked = jnp.concatenate([high, low], axis=0)
        parts = []
        for k in range(1, cols + 1):
            at = pl.multiple_of((my_col + k) % cols * half_y, half_y)
            table = jnp.concatenate([hy[pl.ds(at, half_y), :], hy[pl.ds(ny + at, half_y), :]], axis=0)
            both = jnp.dot(table, stacked, preferred_element_type=F32)
            parts.append(both[:half_y] + both[half_y:])
        for k in range(1, cols):
            mixed[piece, (my_col + k) % cols] = parts[k - 1]
        for k in range(1, cols):
            col_copy(piece, (my_col + k) % cols).start()
        if piece < pieces - 1:
            gathered[piece, my_col] = parts[-1]
        else:
            lines[my_col] = parts[-1]

    for piece in everything:
        with jax.named_scope(f"colwait{piece}"):
            col_all(piece).wait_recv()
        if piece < pieces - 1:
            last_axis(gathered.at[piece], scale[piece % quads], wz, early.at[piece])
        if piece == pieces - 2:
            sent = send.at[:, pl.ds(0, rows - 1)]
            pltpu.make_async_copy(sent, sent, row_send).wait()
    sent = mixed.at[:, pl.ds(0, cols - 1)]
    pltpu.make_async_copy(sent, sent, col_send).wait()


def last_axis(lines, scale, wz, out):
    cols, half_y, _ = lines.shape
    width, _, nz = out.shape
    line = jnp.concatenate([lines[c] for c in range(cols)], axis=1)
    high, low = split(line)
    both = jnp.dot(jnp.concatenate([high, low], axis=0), wz[0], preferred_element_type=F32)
    done = both[:half_y] + both[half_y:]
    done = done + jnp.dot(high, wz[1], preferred_element_type=F32)
    done = done * scale
    for j in range(width):
        out[j] = done[:, j * padded(nz) : j * padded(nz) + nz]


def last_kernel(lines, scale, early, wz, out, held, out_sem):
    pieces = early.shape[0] + 1
    quads, width = scale.shape[0], held.shape[0]
    copies = []
    for piece in range(pieces):
        if piece == pieces - 1:
            last_axis(lines, scale[piece % quads], wz, held)
        source = early.at[piece] if piece < pieces - 1 else held
        place = out.at[piece // quads, pl.ds(piece % quads * width, width)]
        copy = pltpu.make_async_copy(source, place, out_sem.at[piece])
        copy.start()
        copies.append(copy)
    with jax.named_scope("outwait"):
        for copy in copies:
            copy.wait()


def on_device(rows, cols, species, symbol_x, symbol_y, symbol_z):
    fields, nx, share_y, share_z = species.shape
    ny, nz = symbol_y.shape[0], symbol_z.shape[0]
    share_x, half_y = nx // rows, ny // cols
    width = LANES // share_z
    quads = share_x // width
    pieces = fields * quads
    hx, hy, wz = (jnp.asarray(t) for t in tables(rows, nx, ny, nz, share_z))
    dma = pltpu.SemaphoreType.DMA
    regular = pltpu.SemaphoreType.REGULAR
    width_z = width * padded(nz)
    vmem = pl.BlockSpec(memory_space=pltpu.VMEM)
    lines, scale, early = pl.pallas_call(
        functools.partial(kernel, rows, cols, ("row", "col")),
        out_shape=(
            jax.ShapeDtypeStruct((cols, half_y, LANES), F32),
            jax.ShapeDtypeStruct((quads, half_y, width_z), F32),
            jax.ShapeDtypeStruct((pieces - 1, width, half_y, nz), F32),
        ),
        in_specs=[pl.BlockSpec(memory_space=pl.ANY)] * 7,
        out_specs=(vmem, vmem, vmem),
        scratch_shapes=[
            pltpu.VMEM((fields, nx // LANES, share_z, share_y, LANES), F32),
            pltpu.VMEM((fields, share_y * share_z, 2 * nx), F32),
            pltpu.VMEM(hx.shape, BF16),
            pltpu.VMEM(hy.shape, BF16),
            pltpu.VMEM(wz.shape, BF16),
            pltpu.VMEM((1, nx), F32),
            pltpu.VMEM((1, ny), F32),
            pltpu.VMEM((1, nz), F32),
            pltpu.VMEM((pieces, rows, share_y, LANES), F32),
            pltpu.VMEM((pieces, rows, share_y, LANES), F32),
            pltpu.VMEM((pieces, cols, half_y, LANES), F32),
            pltpu.VMEM((pieces - 1, cols, half_y, LANES), F32),
            pltpu.VMEM((nx, LANES), F32),
            pltpu.VMEM((ny, LANES), F32),
            dma,
            dma((pieces,)),
            dma,
            dma((pieces,)),
            regular((3,)),
        ],
        compiler_params=pltpu.CompilerParams(collective_id=0, has_side_effects=True, vmem_limit_bytes=24 * 2**20),
    )(
        *(pltpu.with_memory_space_constraint(v, pltpu.HBM) for v in (jnp.transpose(species, (0, 2, 3, 1)), hx, hy,
        wz, symbol_x[None, :], symbol_y[None, :], symbol_z[None, :])),
    )
    return pl.pallas_call(
        last_kernel,
        out_shape=jax.ShapeDtypeStruct((fields, share_x, half_y, nz), F32),
        in_specs=[vmem, vmem, vmem, vmem],
        out_specs=pl.BlockSpec(memory_space=pl.ANY),
        scratch_shapes=[pltpu.VMEM((width, half_y, nz), F32), dma((pieces,))],
        compiler_params=pltpu.CompilerParams(vmem_limit_bytes=24 * 2**20),
    )(lines, scale, early, wz)


def solution(mesh):
    rows, cols = mesh.shape["row"], mesh.shape["col"]
    in_specs = (P(None, None, "row", "col"), P(), P(), P())
    out_specs = P(None, "row", "col", None)
    return jax.shard_map(
        functools.partial(on_device, rows, cols),
        mesh=mesh, in_specs=in_specs, out_specs=out_specs, check_vma=False,
    )
```
